16 devices in a mesh: data: 2 (over y, z), tensor: 8 (over x, core).
Axes of the slice: x: 4, y: 2, z: 1, core: 2. Of those that a mesh axis runs over, the one named last changes fastest.
The devices are a block of a 4x4x8 slice.
Arguments:
- x_in: bfloat16 [128, 128, 2048], P('data'), parts along dimension 0
- adapter_ids: int32 [128], P('data'), parts along dimension 0
- gain_attn: float32 [2048], replicated
- gain_mlp: float32 [2048], replicated
- w_q: bfloat16 [2048, 32, 64], P(None, 'tensor')
- w_k: bfloat16 [2048, 8, 64], P(None, 'tensor')
- w_v: bfloat16 [2048, 8, 64], P(None, 'tensor')
- w_o: bfloat16 [32, 64, 2048], P('tensor')
- w_gate: bfloat16 [2048, 8192], P(None, 'tensor')
- w_up: bfloat16 [2048, 8192], P(None, 'tensor')
- w_down: bfloat16 [8192, 2048], P('tensor')
- a_q: bfloat16 [2, 2048, 256], P(None, None, 'tensor')
- b_q: bfloat16 [2, 256, 32, 64], P(None, None, 'tensor')
- a_k: bfloat16 [2, 2048, 256], P(None, None, 'tensor')
- b_k: bfloat16 [2, 256, 8, 64], P(None, None, 'tensor')
- a_v: bfloat16 [2, 2048, 256], P(None, None, 'tensor')
- b_v: bfloat16 [2, 256, 8, 64], P(None, None, 'tensor')
- a_o: bfloat16 [2, 32, 64, 256], P(None, 'tensor')
- b_o: bfloat16 [2, 256, 2048], P(None, None, 'tensor')
- a_gate: bfloat16 [2, 2048, 256], P(None, None, 'tensor')
- b_gate: bfloat16 [2, 256, 8192], P(None, None, 'tensor')
- a_up: bfloat16 [2, 2048, 256], P(None, None, 'tensor')
- b_up: bfloat16 [2, 256, 8192], P(None, None, 'tensor')
- a_down: bfloat16 [2, 8192, 256], P(None, 'tensor')
- b_down: bfloat16 [2, 256, 2048], P(None, None, 'tensor')
Outputs:
- output: bfloat16 [128, 128, 2048], P('data'), parts along dimension 0
There are 2 independent parts. The reference program is written for one: setup_inputs(seed, part) draws one part's arguments, and reference() takes and returns one part's arrays. A program takes and returns all parts, laid end to end along the dimension named above; an argument that names none is the same for every part.
All inputs are finite; a program needn't handle non-finite values.
Results may differ from the reference program's by a relative error of at most 0.02.
Values are sent between devices in bfloat16 or wider.
A program may use at most 768 MiB of HBM per device.

```python
import jax
import jax.numpy as jnp
from jax import lax

MODEL_DIM = 2048
FFN_DIM = 8192
NUM_HEADS = 32
KV_HEADS = 8
HEAD_DIM = 64
BATCH = 64
SEQ_LEN = 128
RANK = 256
ADAPTERS = 2
ALPHA = 16
ROPE_BASE = 10000

Q_WIDTH = NUM_HEADS * HEAD_DIM
KV_WIDTH = KV_HEADS * HEAD_DIM
GROUP_SIZE = NUM_HEADS // KV_HEADS
LORA_SCALE = ALPHA / RANK
EPSILON = 1e-5


def draw_ids(key_in):
    key_first, key_second, key_perm = jax.random.split(key_in, 3)
    first_draw = jax.random.randint(key_first, (BATCH,), 0, ADAPTERS)
    second_draw = jax.random.randint(key_second, (BATCH,), 0, ADAPTERS)
    slot_index = jnp.arange(BATCH)
    chosen = jnp.where(slot_index < ADAPTERS, slot_index, jnp.minimum(first_draw, second_draw))
    return jax.random.permutation(key_perm, chosen).astype(jnp.int32)


def setup_inputs(seed: int = 0, part: int = 0) -> dict:
    root_key = jax.random.key(seed)
    key_x, key_ids = jax.random.split(jax.random.fold_in(root_key, part), 2)
    key_list = jax.random.split(root_key, 23)
    b_scale = 0.2 * RANK ** 0.5 / ALPHA

    def normal_bf16(key_in, arr_shape, scale_val):
        return (jax.random.normal(key_in, arr_shape, jnp.float32) * scale_val).astype(jnp.bfloat16)

    return {
        'x_in': normal_bf16(key_x, (BATCH, SEQ_LEN, MODEL_DIM), 1.0),
        'adapter_ids': draw_ids(key_ids),
        'gain_attn': 1.0 + 0.25 * jax.random.normal(key_list[0], (MODEL_DIM,), jnp.float32),
        'gain_mlp': 1.0 + 0.25 * jax.random.normal(key_list[1], (MODEL_DIM,), jnp.float32),
        'w_q': normal_bf16(key_list[2], (MODEL_DIM, NUM_HEADS, HEAD_DIM), 1.6 * MODEL_DIM ** -0.5),
        'w_k': normal_bf16(key_list[3], (MODEL_DIM, KV_HEADS, HEAD_DIM), 1.6 * MODEL_DIM ** -0.5),
        'w_v': normal_bf16(key_list[4], (MODEL_DIM, KV_HEADS, HEAD_DIM), MODEL_DIM ** -0.5),
        'w_o': normal_bf16(key_list[5], (NUM_HEADS, HEAD_DIM, MODEL_DIM), 1.4 * Q_WIDTH ** -0.5),
        'w_gate': normal_bf16(key_list[6], (MODEL_DIM, FFN_DIM), MODEL_DIM ** -0.5),
        'w_up': normal_bf16(key_list[7], (MODEL_DIM, FFN_DIM), MODEL_DIM ** -0.5),
        'w_down': normal_bf16(key_list[8], (FFN_DIM, MODEL_DIM), 1.4 * FFN_DIM ** -0.5),
        'a_q': normal_bf16(key_list[9], (ADAPTERS, MODEL_DIM, RANK), MODEL_DIM ** -0.5),
        'b_q': normal_bf16(key_list[10], (ADAPTERS, RANK, NUM_HEADS, HEAD_DIM), 1.6 * b_scale),
        'a_k': normal_bf16(key_list[11], (ADAPTERS, MODEL_DIM, RANK), MODEL_DIM ** -0.5),
        'b_k': normal_bf16(key_list[12], (ADAPTERS, RANK, KV_HEADS, HEAD_DIM), 1.6 * b_scale),
        'a_v': normal_bf16(key_list[13], (ADAPTERS, MODEL_DIM, RANK), MODEL_DIM ** -0.5),
        'b_v': normal_bf16(key_list[14], (ADAPTERS, RANK, KV_HEADS, HEAD_DIM), b_scale),
        'a_o': normal_bf16(key_list[15], (ADAPTERS, NUM_HEADS, HEAD_DIM, RANK), Q_WIDTH ** -0.5),
        'b_o': normal_bf16(key_list[16], (ADAPTERS, RANK, MODEL_DIM), 1.4 * b_scale),
        'a_gate': normal_bf16(key_list[17], (ADAPTERS, MODEL_DIM, RANK), MODEL_DIM ** -0.5),
        'b_gate': normal_bf16(key_list[18], (ADAPTERS, RANK, FFN_DIM), b_scale),
        'a_up': normal_bf16(key_list[19], (ADAPTERS, MODEL_DIM, RANK), MODEL_DIM ** -0.5),
        'b_up': normal_bf16(key_list[20], (ADAPTERS, RANK, FFN_DIM), b_scale),
        'a_down': normal_bf16(key_list[21], (ADAPTERS, FFN_DIM, RANK), FFN_DIM ** -0.5),
        'b_down': normal_bf16(key_list[22], (ADAPTERS, RANK, MODEL_DIM), 1.4 * b_scale),
    }


def rms_gain(act_in, gain_vec):
    act_f32 = act_in.astype(jnp.float32)
    inv_rms = lax.rsqrt(jnp.mean(act_f32 * act_f32, axis=-1, keepdims=True) + EPSILON)
    return (act_f32 * inv_rms * gain_vec).astype(jnp.bfloat16)


def rope_rotate(head_vals):
    half_dim = HEAD_DIM // 2
    inv_freq = ROPE_BASE ** (-2.0 * jnp.arange(half_dim, dtype=jnp.float32) / HEAD_DIM)
    angle_tab = jnp.arange(SEQ_LEN, dtype=jnp.float32)[:, None] * inv_freq[None, :]
    cos_tab = jnp.cos(angle_tab)[:, None, :]
    sin_tab = jnp.sin(angle_tab)[:, None, :]
    first_half = head_vals[..., :half_dim]
    second_half = head_vals[..., half_dim:]
    return jnp.concatenate([first_half * cos_tab - second_half * sin_tab, second_half * cos_tab + first_half * sin_tab], axis=-1)


def reference(x_in, adapter_ids, gain_attn, gain_mlp, w_q, w_k, w_v, w_o, w_gate, w_up, w_down, a_q, b_q, a_k, b_k, a_v, b_v, a_o, b_o, a_gate, b_gate, a_up, b_up, a_down, b_down):
    flat_q = w_q.reshape(MODEL_DIM, Q_WIDTH)
    flat_k = w_k.reshape(MODEL_DIM, KV_WIDTH)
    flat_v = w_v.reshape(MODEL_DIM, KV_WIDTH)
    flat_o = w_o.reshape(Q_WIDTH, MODEL_DIM)
    causal = jnp.arange(SEQ_LEN)[:, None] >= jnp.arange(SEQ_LEN)[None, :]

    def project(act_in, weight, a_mat, b_mat):
        base_out = jnp.dot(act_in, weight, preferred_element_type=jnp.float32)
        low_rank = jnp.dot(act_in, a_mat, preferred_element_type=jnp.float32).astype(jnp.bfloat16)
        return base_out + LORA_SCALE * jnp.dot(low_rank, b_mat, preferred_element_type=jnp.float32)

    def one_sequence(seq_pair):
        x_seq, adapter = seq_pair
        h_attn = rms_gain(x_seq, gain_attn)
        z_q = project(h_attn, flat_q, a_q[adapter], b_q[adapter].reshape(RANK, Q_WIDTH))
        z_k = project(h_attn, flat_k, a_k[adapter], b_k[adapter].reshape(RANK, KV_WIDTH))
        z_v = project(h_attn, flat_v, a_v[adapter], b_v[adapter].reshape(RANK, KV_WIDTH))
        q_heads = rope_rotate(z_q.reshape(SEQ_LEN, NUM_HEADS, HEAD_DIM)).astype(jnp.bfloat16)
        k_heads = rope_rotate(z_k.reshape(SEQ_LEN, KV_HEADS, HEAD_DIM)).astype(jnp.bfloat16)
        v_heads = z_v.reshape(SEQ_LEN, KV_HEADS, HEAD_DIM).astype(jnp.bfloat16)
        q_group = q_heads.reshape(SEQ_LEN, KV_HEADS, GROUP_SIZE, HEAD_DIM)
        scores = jnp.einsum('skgd,tkd->kgst', q_group.astype(jnp.float32), k_heads.astype(jnp.float32)) * HEAD_DIM ** -0.5
        attn_prob = jax.nn.softmax(jnp.where(causal, scores, -1e30), axis=-1).astype(jnp.bfloat16)
        mixed_out = jnp.einsum('kgst,tkd->skgd', attn_prob.astype(jnp.float32), v_heads.astype(jnp.float32))
        attn_out = mixed_out.astype(jnp.bfloat16).reshape(SEQ_LEN, Q_WIDTH)
        z_o = project(attn_out, flat_o, a_o[adapter].reshape(Q_WIDTH, RANK), b_o[adapter])
        x_mid = (x_seq.astype(jnp.float32) + z_o).astype(jnp.bfloat16)
        h_mlp = rms_gain(x_mid, gain_mlp)
        z_gate = project(h_mlp, w_gate, a_gate[adapter], b_gate[adapter])
        z_up = project(h_mlp, w_up, a_up[adapter], b_up[adapter])
        hidden = (jax.nn.silu(z_gate) * z_up).astype(jnp.bfloat16)
        z_down = project(hidden, w_down, a_down[adapter], b_down[adapter])
        return (x_mid.astype(jnp.float32) + z_down).astype(jnp.bfloat16)

    return lax.map(one_sequence, (x_in, adapter_ids))
```

```python
import functools

import jax
import jax.numpy as jnp
from jax import lax
from jax.experimental import pallas as pl
from jax.experimental.pallas import tpu as pltpu
from jax.sharding import PartitionSpec as P

ALPHA = 16.0
ROPE_BASE = 10000.0
EPSILON = 1e-5
CORES = 2
CHUNKS = 4
VMEM_LIMIT = 62 * 1024 * 1024
F32, BF16 = jnp.float32, jnp.bfloat16


def dot_nn(a, b):
    return lax.dot_general(a, b, (((1,), (0,)), ((), ())), preferred_element_type=F32)


def dot_nt(a, b):
    return lax.dot_general(a, b, (((1,), (1,)), ((), ())), preferred_element_type=F32)


def norm_tile(load_rows, gain_ref, dst_ref, n_rows):
    step_rows = 16

    @pl.loop(0, n_rows // step_rows)
    def _(i):
        v = load_rows(i, step_rows).astype(F32)
        inv = lax.rsqrt(jnp.mean(v * v, axis=-1, keepdims=True) + EPSILON)
        rows = pl.ds(pl.multiple_of(i * step_rows, step_rows), step_rows)
        dst_ref[rows, :] = (v * inv * gain_ref[...]).astype(BF16)


def attn_body(dims, meta, x_ref, gain_ref, cosq_ref, sinq_ref, cosk_ref, sink_ref,
              gw_ref, aqkv_ref, gb_ref, gwo_ref, out_ref,
              wq, wk, wv, aq, bq, bk, bv, wo, ao, bo, h_scr, low_scr, k_scr, v_scr, attn_scr, sems):
    n_dev, seqs, S, hd, nq, rank, D, spc, base_step, chips = dims
    half = hd // 2
    qw = nq * hd
    scale = ALPHA / rank
    step = pl.program_id(0)
    core = meta[meta.shape[0] - 1]

    plans = [[], [], [], []]
    plans[0].append((aqkv_ref, aq))
    for d in range(n_dev):
        plans[1].append((gw_ref.at[d, pl.ds(qw, half)], wk.at[pl.ds(d * half, half)]))
        plans[1].append((gw_ref.at[d, pl.ds(qw + half, half)], wk.at[pl.ds((n_dev + d) * half, half)]))
        plans[1].append((gw_ref.at[d, pl.ds(qw + hd, hd)], wv.at[pl.ds(d * hd, hd)]))
        for a in range(2):
            o = a * (qw + 2 * hd)
            plans[1].append((gb_ref.at[d, pl.ds(o + qw, half)], bk.at[a, pl.ds(d * half, half)]))
            plans[1].append((gb_ref.at[d, pl.ds(o + qw + half, half)], bk.at[a, pl.ds((n_dev + d) * half, half)]))
            plans[1].append((gb_ref.at[d, pl.ds(o + qw + hd, hd)], bv.at[a, pl.ds(d * hd, hd)]))
    for d in range(n_dev):
        plans[2].append((gw_ref.at[d, pl.ds(0, qw)], wq.at[pl.ds(d * qw, qw)]))
        for a in range(2):
            o = a * (qw + 2 * hd)
            plans[2].append((gb_ref.at[d, pl.ds(o, qw)], bq.at[a, pl.ds(d * qw, qw)]))
    off = 2 * (qw + 2 * hd)
    for d in range(n_dev):
        plans[3].append((gwo_ref.at[d], wo.at[pl.ds(d * qw, qw)]))
        for a in range(2):
            plans[3].append((gb_ref.at[d, pl.ds(off + a * qw, qw)], ao.at[a, pl.ds(d * qw, qw)]))
            plans[3].append((gb_ref.at[d, pl.ds(off + 2 * qw + a * rank, rank)],
                             bo.at[a, :, pl.ds(d * qw, qw)]))

    @pl.when(step == 0)
    def _():
        for i, plan in enumerate(plans):
            for src, dst in plan:
                pltpu.make_async_copy(src, dst, sems.at[i]).start()

    def arrive(i):
        @pl.when(step == 0)
        def _():
            for src, dst in plans[i]:
                pltpu.make_async_copy(src, dst, sems.at[i]).wait()

    per = seqs // chips
    ids = [meta[t * per + core * (per // CORES) + base_step + step] for t in range(chips)]
    M = chips * S

    def load_x(i, n):
        t = i // (S // n)
        r = i % (S // n)
        return x_ref[t, 0, pl.ds(pl.multiple_of(r * n, n), n), :]

    norm_tile(load_x, gain_ref, h_scr, M)
    arrive(0)
    for t in range(chips):
        low_scr[pl.ds(t * S, S), :] = dot_nn(h_scr[pl.ds(t * S, S), :], aq[ids[t]]).astype(BF16)
    arrive(1)
    kh = n_dev * half
    zk = dot_nt(h_scr[...], wk[...])
    for t in range(chips):
        z = zk[t * S:(t + 1) * S] + scale * dot_nt(low_scr[pl.ds(t * S, S), rank:2 * rank], bk[ids[t]])
        f, s = z[:, :kh], z[:, kh:]
        k_scr[pl.ds(t * S, S), :kh] = (f * cosk_ref[...] - s * sink_ref[...]).astype(BF16).astype(F32)
        k_scr[pl.ds(t * S, S), kh:] = (s * cosk_ref[...] + f * sink_ref[...]).astype(BF16).astype(F32)
    zv = dot_nt(h_scr[...], wv[...])
    for t in range(chips):
        z = zv[t * S:(t + 1) * S] + scale * dot_nt(low_scr[pl.ds(t * S, S), 2 * rank:], bv[ids[t]])
        v_scr[pl.ds(t * S, S), :] = z.astype(BF16).astype(F32)
    arrive(2)

    lanes = nq * half
    per_vreg = lanes // half
    per_v = lanes // hd

    @pl.loop(0, n_dev)
    def _(g):
        zq = dot_nt(h_scr[...], wq[pl.ds(pl.multiple_of(g * qw, qw), qw), :])
        lane = lax.broadcasted_iota(jnp.int32, (S, lanes), 1)
        row = lax.broadcasted_iota(jnp.int32, (S, S), 0)
        col = lax.broadcasted_iota(jnp.int32, (S, S), 1)
        causal = col <= row
        kbase = pl.multiple_of((g // per_vreg) * lanes, lanes)
        vbase = pl.multiple_of((g // per_v) * lanes, lanes)
        mine_k = (lane // half) == (g % per_vreg)
        mine_v = (lane // hd) == (g % per_v)
        for t in range(chips):
            rows = pl.ds(t * S, S)
            z = zq[t * S:(t + 1) * S] + scale * dot_nt(
                low_scr[rows, :rank], bq[ids[t], pl.ds(pl.multiple_of(g * qw, qw), qw), :])
            f, s = z[:, :lanes], z[:, lanes:]
            q = jnp.concatenate([(f * cosq_ref[...] - s * sinq_ref[...]).astype(BF16),
                                 (s * cosq_ref[...] + f * sinq_ref[...]).astype(BF16)], axis=1)

            def spread(v, mine, width):
                v = jnp.where(mine, v, 0.0)
                while width < lanes:
                    v = v + pltpu.roll(v, width, axis=1)
                    width *= 2
                return v

            kf = spread(k_scr[rows, pl.ds(kbase, lanes)], mine_k, half)
            ks = spread(k_scr[rows, pl.ds(kh + kbase, lanes)], mine_k, half)
            vv = spread(v_scr[rows, pl.ds(vbase, lanes)], mine_v, hd)
            kd, vd = [], []
            for hh in range(nq):
                sel = (lane // half) == hh
                kd.append(jnp.concatenate([jnp.where(sel, kf, 0.0).astype(BF16),
                                           jnp.where(sel, ks, 0.0).astype(BF16)], axis=1))
                parts = []
                for w in range(qw // lanes):
                    if hh // per_v == w:
                        parts.append(jnp.where((lane // hd) == (hh % per_v), vv, 0.0).astype(BF16))
                    else:
                        parts.append(jnp.zeros((S, lanes), BF16))
                vd.append(jnp.concatenate(parts, axis=1))
            sc = dot_nt(q, jnp.concatenate(kd, axis=0))
            ps = []
            for hh in range(nq):
                sh = jnp.where(causal, sc[:, hh * S:(hh + 1) * S], -1e30)
                e = jnp.exp(sh - jnp.max(sh, axis=1, keepdims=True))
                ps.append((e * (1.0 / jnp.sum(e, axis=1, keepdims=True))).astype(BF16))
            o = dot_nn(jnp.concatenate(ps, axis=1), jnp.concatenate(vd, axis=0))
            attn_scr[rows, pl.ds(pl.multiple_of(g * qw, qw), qw)] = o.astype(BF16)

    arrive(3)
    for t in range(chips):
        low_scr[pl.ds(t * S, S), :rank] = dot_nn(attn_scr[pl.ds(t * S, S), :], ao[ids[t]]).astype(BF16)
    nt = 256

    @pl.loop(0, D // nt)
    def _(j):
        cols = pl.ds(pl.multiple_of(j * nt, nt), nt)
        zo = dot_nn(attn_scr[...], wo[:, cols])
        for t in range(chips):
            z = zo[t * S:(t + 1) * S] + scale * dot_nn(low_scr[pl.ds(t * S, S), :rank], bo[ids[t], :, cols])
            out_ref[t, :, cols] = (x_ref[t, 0, :, cols].astype(F32) + z).astype(BF16)


def mlp_body(dims, meta, x_ref, gain_ref, agu_ref, wg0, wg1, wu0, wu1, wd0, wd1, bg0, bg1, bu0, bu1, ad0, ad1,
             out_ref, wg, wu, wd, bg, bu, agu, ad, h_scr, low_scr, hid_scr, sems):
    seqs, S, rank, D, spc, base_step, chips = dims
    scale = ALPHA / rank
    step = pl.program_id(0)
    core = meta[meta.shape[0] - 1]
    fw = wg0.shape[1]
    plans = [[(agu_ref, agu)], [], []]
    for i, (g, u, b1, b2) in enumerate(((wg0, wu0, bg0, bu0), (wg1, wu1, bg1, bu1))):
        c = pl.ds(i * fw, fw)
        plans[1] += [(g, wg.at[:, c]), (u, wu.at[:, c]), (b1, bg.at[:, :, c]), (b2, bu.at[:, :, c])]
    for i, (d, a) in enumerate(((wd0, ad0), (wd1, ad1))):
        c = pl.ds(i * fw, fw)
        plans[2] += [(a, ad.at[:, c]), (d, wd.at[c])]

    @pl.when(step == 0)
    def _():
        for i, plan in enumerate(plans):
            for src, dst in plan:
                pltpu.make_async_copy(src, dst, sems.at[i]).start()

    def arrive(i):
        @pl.when(step == 0)
        def _():
            for src, dst in plans[i]:
                pltpu.make_async_copy(src, dst, sems.at[i]).wait()

    per = seqs // chips
    ids = [meta[t * per + core * (per // CORES) + base_step + step] for t in range(chips)]
    M = chips * S

    def load_x(i, n):
        t = i // (S // n)
        r = i % (S // n)
        return x_ref[t, pl.ds(pl.multiple_of(r * n, n), n), :]

    norm_tile(load_x, gain_ref, h_scr, M)
    arrive(0)
    for t in range(chips):
        low_scr[pl.ds(t * S, S), :] = dot_nn(h_scr[pl.ds(t * S, S), :], agu[ids[t]]).astype(BF16)
    arrive(1)
    nt = 256

    @pl.loop(0, wg.shape[1] // nt)
    def _(j):
        cols = pl.ds(pl.multiple_of(j * nt, nt), nt)
        zg = dot_nn(h_scr[...], wg[:, cols])
        zu = dot_nn(h_scr[...], wu[:, cols])
        for t in range(chips):
            rows = pl.ds(t * S, S)
            g = zg[t * S:(t + 1) * S] + scale * dot_nn(low_scr[rows, :rank], bg[ids[t], :, cols])
            u = zu[t * S:(t + 1) * S] + scale * dot_nn(low_scr[rows, rank:], bu[ids[t], :, cols])
            hid_scr[rows, cols] = (jax.nn.silu(g) * u).astype(BF16)

    arrive(2)
    for t in range(chips):
        out_ref[t, :, D:] = dot_nn(hid_scr[pl.ds(t * S, S), :], ad[ids[t]]).astype(BF16)

    @pl.loop(0, D // nt)
    def _(j):
        cols = pl.ds(pl.multiple_of(j * nt, nt), nt)
        z = dot_nn(hid_scr[...], wd[:, cols])
        for t in range(chips):
            out_ref[t, :, cols] = z[t * S:(t + 1) * S].astype(BF16)


def finish_body(dims, meta, x_ref, rs_ref, bd_ref, out_ref):
    rank, D = dims
    scale = ALPHA / rank
    nt = 256
    low = rs_ref[0, :, D:]

    @pl.loop(0, D // nt)
    def _(j):
        cols = pl.ds(pl.multiple_of(j * nt, nt), nt)
        delta = scale * dot_nn(low, bd_ref[0, :, cols])
        out_ref[0, :, cols] = (x_ref[0, 0, :, cols].astype(F32) + rs_ref[0, :, cols].astype(F32) + delta).astype(BF16)


def solution(mesh):
    n_dev = mesh.shape['tensor']
    chips = n_dev // CORES
    head_split = P(None, 'tensor', None)
    last_split = P(None, None, 'tensor')
    b_head_split = P(None, None, 'tensor', None)
    in_specs = (P('data', None, None), P('data'), P(None), P(None),
                head_split, head_split, head_split, P('tensor', None, None),
                P(None, 'tensor'), P(None, 'tensor'), P('tensor', None),
                last_split, b_head_split, last_split, b_head_split, last_split, b_head_split,
                P(None, 'tensor', None, None), last_split,
                last_split, last_split, last_split, last_split,
                P(None, 'tensor', None), last_split)
    same_core = [[c + CORES * i for i in range(chips)] for c in range(CORES)]
    swap = [(i, i ^ 1) for i in range(n_dev)]
    ANY = pl.BlockSpec(memory_space=pl.ANY)

    def local_layer(x_in, adapter_ids, gain_attn, gain_mlp, w_q, w_k, w_v, w_o, w_gate, w_up, w_down, a_q, b_q, a_k, b_k, a_v, b_v, a_o, b_o, a_gate, b_gate, a_up, b_up, a_down, b_down):
        seqs, S, D = x_in.shape
        nq, hd = w_q.shape[1], w_q.shape[2]
        n_ad, rank = b_q.shape[0], b_q.shape[1]
        rl = a_q.shape[2]
        half = hd // 2
        qw = nq * hd
        me = lax.axis_index('tensor')
        core, chip = me % CORES, me // CORES
        meta = jnp.concatenate([adapter_ids.astype(jnp.int32), core.reshape(1).astype(jnp.int32)])
        per = seqs // chips
        steps = per // CORES
        spc = steps // CHUNKS

        def rows_t(w):
            return jnp.transpose(w, (1, 2, 0)).reshape(-1, w.shape[0])

        def split_halves(wt, heads):
            return wt.reshape(heads, 2, half, -1).transpose(1, 0, 2, 3).reshape(heads * hd, -1)

        gather = functools.partial(lax.all_gather, axis_name='tensor', axis=0)
        swapped = functools.partial(lax.ppermute, axis_name='tensor', perm=swap)

        g_a = gather(jnp.concatenate([jnp.transpose(a, (0, 2, 1)).reshape(n_ad * rl, D)
                                      for a in (a_q, a_k, a_v, a_gate, a_up)], axis=0))
        g_a = g_a.reshape(n_dev, 5, n_ad, rl, D)
        a_qkv = g_a[:, :3].transpose(2, 4, 1, 0, 3).reshape(n_ad, D, 3 * rank)
        a_gu = g_a[:, 3:].transpose(2, 4, 1, 0, 3).reshape(n_ad, D, 2 * rank)
        g_w = gather(jnp.concatenate([split_halves(rows_t(w_q), nq), rows_t(w_k), rows_t(w_v)], axis=0))

        def b_rows(b):
            return jnp.transpose(b, (1, 2, 0)).reshape(-1, rank)

        b_parts = []
        for a in range(n_ad):
            b_parts += [split_halves(b_rows(b_q[a]), nq), b_rows(b_k[a]), b_rows(b_v[a])]
        b_parts += [a_o.reshape(n_ad * qw, rank), b_o.reshape(n_ad * rank, qw)]
        g_b = gather(jnp.concatenate(b_parts, axis=0))
        g_wo = gather(w_o.reshape(qw, D))
        g_bd = gather(b_down.reshape(n_ad * rank, qw))
        bd_full = g_bd.reshape(n_dev, n_ad, rank, qw).transpose(1, 2, 0, 3).reshape(n_ad, rank, D)
        mlp_own = (w_gate, w_up, w_down, b_gate, b_up, a_down)
        mlp_other = tuple(swapped(w) for w in mlp_own)

        inv_freq = ROPE_BASE ** (-2.0 * jnp.arange(half, dtype=F32) / hd)
        ang = jnp.arange(S, dtype=F32)[:, None] * inv_freq[None, :]
        cos, sin = jnp.cos(ang), jnp.sin(ang)
        qs = hd ** -0.5
        cosq, sinq = jnp.tile(cos, (1, nq)) * qs, jnp.tile(sin, (1, nq)) * qs
        cosk, sink = jnp.tile(cos, (1, n_dev)), jnp.tile(sin, (1, n_dev))

        x4 = x_in.reshape(chips, per, S, D)
        M = chips * S
        Fc = CORES * w_gate.shape[1]
        full = lambda shape: pl.BlockSpec(shape, lambda i, m: (0,) * len(shape))
        params = pltpu.CompilerParams(vmem_limit_bytes=VMEM_LIMIT, dimension_semantics=("arbitrary",))
        y = jnp.zeros((n_dev, steps * S, D), BF16)
        for c in range(CHUNKS):
            base_step = c * spc
            tok = M * spc
            x1 = pl.pallas_call(
                functools.partial(attn_body, (n_dev, seqs, S, hd, nq, rank, D, spc, base_step, chips)),
                grid_spec=pltpu.PrefetchScalarGridSpec(
                    num_scalar_prefetch=1, grid=(spc,),
                    in_specs=[pl.BlockSpec((chips, 1, S, D), lambda i, m, b=base_step: (0, m[seqs] * steps + b + i, 0, 0)),
                              full((1, D)), full((S, nq * half)), full((S, nq * half)),
                              full((S, n_dev * half)), full((S, n_dev * half)), ANY, ANY, ANY, ANY],
                    out_specs=pl.BlockSpec((chips, S, D), lambda i, m: (0, i, 0)),
                    scratch_shapes=[
                        pltpu.VMEM((n_dev * qw, D), BF16), pltpu.VMEM((n_dev * hd, D), BF16), pltpu.VMEM((n_dev * hd, D), BF16),
                        pltpu.VMEM((n_ad, D, 3 * rank), BF16),
                        pltpu.VMEM((n_ad, n_dev * qw, rank), BF16), pltpu.VMEM((n_ad, n_dev * hd, rank), BF16),
                        pltpu.VMEM((n_ad, n_dev * hd, rank), BF16),
                        pltpu.VMEM((n_dev * qw, D), BF16), pltpu.VMEM((n_ad, n_dev * qw, rank), BF16),
                        pltpu.VMEM((n_ad, rank, n_dev * qw), BF16),
                        pltpu.VMEM((M, D), BF16), pltpu.VMEM((M, 3 * rank), BF16),
                        pltpu.VMEM((M, n_dev * hd), F32), pltpu.VMEM((M, n_dev * hd), F32),
                        pltpu.VMEM((M, n_dev * qw), BF16), pltpu.SemaphoreType.DMA((4,))]),
                out_shape=jax.ShapeDtypeStruct((chips, spc * S, D), BF16),
                compiler_params=params, name="attn_block",
                cost_estimate=pl.CostEstimate(flops=2 * tok * D * (2 * n_dev * qw + 2 * n_dev * hd + 5 * rank) * 3 // 2,
                                              bytes_accessed=4 * tok * D + 33 * 2**20, transcendentals=0),
            )(meta, x4, gain_attn.reshape(1, D), cosq, sinq, cosk, sink, g_w, a_qkv, g_b, g_wo)
            pairs = [w for own, other in zip(mlp_own, mlp_other) for w in (own, other)]
            part = pl.pallas_call(
                functools.partial(mlp_body, (seqs, S, rank, D, spc, base_step, chips)),
                grid_spec=pltpu.PrefetchScalarGridSpec(
                    num_scalar_prefetch=1, grid=(spc,),
                    in_specs=[pl.BlockSpec((chips, S, D), lambda i, m: (0, i, 0)), full((1, D))] + [ANY] * 13,
                    out_specs=pl.BlockSpec((chips, S, D + rank), lambda i, m: (0, i, 0)),
                    scratch_shapes=[
                        pltpu.VMEM((D, Fc), BF16), pltpu.VMEM((D, Fc), BF16), pltpu.VMEM((Fc, D), BF16),
                        pltpu.VMEM((n_ad, rank, Fc), BF16), pltpu.VMEM((n_ad, rank, Fc), BF16),
                        pltpu.VMEM((n_ad, D, 2 * rank), BF16), pltpu.VMEM((n_ad, Fc, rank), BF16),
                        pltpu.VMEM((M, D), BF16), pltpu.VMEM((M, 2 * rank), BF16), pltpu.VMEM((M, Fc), BF16),
                        pltpu.SemaphoreType.DMA((3,))]),
                out_shape=jax.ShapeDtypeStruct((chips, spc * S, D + rank), BF16),
                compiler_params=params, name="mlp_block",
                cost_estimate=pl.CostEstimate(flops=2 * tok * D * (3 * Fc + 4 * rank),
                                              bytes_accessed=4 * tok * D + 34 * 2**20, transcendentals=tok * Fc),
            )(meta, x1, gain_mlp.reshape(1, D), a_gu, *pairs)
            rs = lax.psum_scatter(part, 'tensor', scatter_dimension=0, axis_index_groups=same_core, tiled=True)
            own = [adapter_ids[chip * per + core * steps + base_step + i] for i in range(spc)]
            meta2 = jnp.concatenate([jnp.stack(own).astype(jnp.int32), chip.reshape(1).astype(jnp.int32)])
            y_own = pl.pallas_call(
                functools.partial(finish_body, (rank, D)),
                grid_spec=pltpu.PrefetchScalarGridSpec(
                    num_scalar_prefetch=1, grid=(spc,),
                    in_specs=[pl.BlockSpec((1, 1, S, D), lambda i, m: (m[spc], i, 0, 0)),
                              pl.BlockSpec((1, S, D + rank), lambda i, m: (i, 0, 0)),
                              pl.BlockSpec((1, rank, D), lambda i, m: (m[i], 0, 0))],
                    out_specs=pl.BlockSpec((1, S, D), lambda i, m: (i, 0, 0))),
                out_shape=jax.ShapeDtypeStruct((spc, S, D), BF16),
                compiler_params=pltpu.CompilerParams(dimension_semantics=("arbitrary",)), name="finish",
                cost_estimate=pl.CostEstimate(flops=2 * spc * S * rank * D, bytes_accessed=10 * spc * S * D, transcendentals=0),
            )(meta2, x1.reshape(chips, spc, S, D), rs.reshape(spc, S, D + rank), bd_full)
            y_all = gather(y_own.reshape(spc * S, D))
            y = lax.dynamic_update_slice(y, y_all, (0, base_step * S, 0))
        return y.reshape(seqs, S, D)

    return jax.shard_map(local_layer, mesh=mesh, in_specs=in_specs, out_specs=P('data', None, None), check_vma=False)
```

```python
import functools

import jax
import jax.numpy as jnp
from jax import lax
from jax.experimental import pallas as pl
from jax.experimental.pallas import tpu as pltpu
from jax.sharding import PartitionSpec as P

ALPHA = 16.0
ROPE_BASE = 10000.0
EPSILON = 1e-5
CORES = 2
CHUNKS = 4
VMEM_LIMIT = 62 * 1024 * 1024
F32, BF16 = jnp.float32, jnp.bfloat16


def dot_nn(a, b):
    return lax.dot_general(a, b, (((1,), (0,)), ((), ())), preferred_element_type=F32)


def dot_nt(a, b):
    return lax.dot_general(a, b, (((1,), (1,)), ((), ())), preferred_element_type=F32)


def norm_tile(load_rows, gain_ref, dst_ref, n_rows):
    step_rows = 16

    @pl.loop(0, n_rows // step_rows)
    def _(i):
        v = load_rows(i, step_rows).astype(F32)
        inv = lax.rsqrt(jnp.mean(v * v, axis=-1, keepdims=True) + EPSILON)
        rows = pl.ds(pl.multiple_of(i * step_rows, step_rows), step_rows)
        dst_ref[rows, :] = (v * inv * gain_ref[...]).astype(BF16)


def attn_body(dims, ids_ref, x_ref, gain_ref, cos_ref, sin_ref, gw_ref, aqkv_ref, gb_ref, gwo_ref, out_ref,
              h, low, attn, w, bw, q_scr, k_scr, v_scr, lowo, wsem, xsem, osem):
    n_dev, seqs, S, hd, nq, rank, D, chips = dims
    half = hd // 2
    qw = nq * hd
    n_ad = 2
    scale = ALPHA / rank
    core = lax.axis_index('tensor') % CORES
    per = seqs // chips
    steps = per // CORES
    M = chips * S
    pw = CORES * (qw + 2 * hd)
    kw = CORES * qw
    vw = kw + CORES * hd

    def seq_id(i, t):
        return ids_ref[t * per + core * steps + i]

    def tile(i):
        return pl.ds(pl.multiple_of(i * M, M), M)

    a_rows = n_ad * 3 * rank
    x_base = 4 * M
    plan_a = [(aqkv_ref, attn.at[pl.ds(0, a_rows)])]
    plan_w = []
    for p in range(chips):
        plan = []
        for c in range(CORES):
            d = p * CORES + c
            plan += [(gw_ref.at[d, pl.ds(0, qw)], w.at[p, pl.ds(c * qw, qw)]),
                     (gw_ref.at[d, pl.ds(qw, hd)], w.at[p, pl.ds(kw + c * hd, hd)]),
                     (gw_ref.at[d, pl.ds(qw + hd, hd)], w.at[p, pl.ds(vw + c * hd, hd)])]
            for a in range(n_ad):
                o = a * (qw + 2 * hd)
                plan += [(gb_ref.at[d, pl.ds(o, qw)], bw.at[p, a, pl.ds(c * qw, qw)]),
                         (gb_ref.at[d, pl.ds(o + qw, hd)], bw.at[p, a, pl.ds(kw + c * hd, hd)]),
                         (gb_ref.at[d, pl.ds(o + qw + hd, hd)], bw.at[p, a, pl.ds(vw + c * hd, hd)])]
        plan_w.append(plan)
    plan_o = []
    off = n_ad * (qw + 2 * hd)
    for d in range(n_dev):
        plan_o.append((gwo_ref.at[d], h.at[pl.ds(d * qw, qw)]))
        for a in range(n_ad):
            plan_o.append((gb_ref.at[d, pl.ds(off + a * qw, qw)], low.at[pl.ds((a * n_dev + d) * qw, qw), pl.ds(0, rank)]))
            plan_o.append((gb_ref.at[d, pl.ds(off + n_ad * qw + a * rank, rank)],
                           h.at[pl.ds(n_dev * qw + a * rank, rank), pl.ds(d * qw, qw)]))

    def start(plan, sem):
        for s, d in plan:
            pltpu.make_async_copy(s, d, sem).start()

    def finish(plan, sem):
        for s, d in plan:
            pltpu.make_async_copy(s, d, sem).wait()

    def x_copies(i, buf, base, slot):
        return [pltpu.make_async_copy(x_ref.at[t, core * steps + i],
                                      buf.at[pl.ds(pl.multiple_of(base + slot * M + t * S, S), S)], xsem.at[slot])
                for t in range(chips)]

    start(plan_a, wsem.at[chips])
    for c in x_copies(0, attn, x_base, 0):
        c.start()
    for p in range(chips):
        start(plan_w[p], wsem.at[p])

    rb = 16

    @pl.loop(0, steps)
    def _(i):
        slot = i % 2
        for c in x_copies(i, attn, x_base, slot):
            c.wait()

        @pl.when(i + 1 < steps)
        def _():
            for c in x_copies(i + 1, attn, x_base, 1 - slot):
                c.start()

        @pl.loop(0, M // rb)
        def _(r):
            v = attn[pl.ds(pl.multiple_of(x_base + slot * M + r * rb, rb), rb), :].astype(F32)
            inv = lax.rsqrt(jnp.mean(v * v, axis=-1, keepdims=True) + EPSILON)
            h[pl.ds(pl.multiple_of(i * M + r * rb, rb), rb), :] = (v * inv * gain_ref[...]).astype(BF16)

        @pl.when(i == 0)
        def _():
            finish(plan_a, wsem.at[chips])
        for t in range(chips):
            rows = pl.ds(pl.multiple_of(i * M + t * S, S), S)
            a = attn[pl.ds(pl.multiple_of(seq_id(i, t) * 3 * rank, 3 * rank), 3 * rank), :]
            low[rows, :] = dot_nt(h[rows, :], a).astype(BF16)

    def produce(it, slot):
        p, i = it // steps, it % steps
        z = dot_nt(w[p], h[tile(i), :])
        for t in range(chips):
            rows = pl.ds(pl.multiple_of(i * M + t * S, S), S)
            b = bw[p, seq_id(i, t)]
            lo = low[rows, :]
            cols = slice(t * S, (t + 1) * S)
            zq = z[:kw, cols] + scale * dot_nt(b[:kw], lo[:, :rank])
            zk = z[kw:vw, cols] + scale * dot_nt(b[kw:vw], lo[:, rank:2 * rank])
            zv = z[vw:, cols] + scale * dot_nt(b[vw:], lo[:, 2 * rank:])
            cos, sin = cos_ref[...], sin_ref[...]

            def rotate(v):
                f, s = v[:half], v[half:]
                return jnp.concatenate([f * cos - s * sin, s * cos + f * sin], axis=0)

            for hh in range(CORES * nq):
                o = hh * hd
                q_scr[slot, o:o + hd, cols] = (rotate(zq[o:o + hd]) * hd ** -0.5).astype(BF16)
            kt = jnp.concatenate([rotate(zk[c * hd:(c + 1) * hd]) for c in range(CORES)], axis=0)
            kk = kt.T.astype(BF16)
            for c in range(CORES):
                k_scr[slot, c, t * S:(t + 1) * S, :] = kk[:, c * hd:(c + 1) * hd]
            v_scr[slot, :, cols] = zv.astype(BF16)

    def consume(it, slot):
        p, i = it // steps, it % steps
        key = lax.broadcasted_iota(jnp.int32, (S, S), 0)
        qry = lax.broadcasted_iota(jnp.int32, (S, S), 1)
        causal = key <= qry
        for c in range(CORES):
            for t in range(chips):
                cols = slice(t * S, (t + 1) * S)
                q = jnp.concatenate([q_scr[slot, c * qw + hh * hd:c * qw + (hh + 1) * hd, cols] for hh in range(nq)], axis=1)
                sc = dot_nn(k_scr[slot, c, cols, :], q)
                ps = []
                for hh in range(nq):
                    sh = jnp.where(causal, sc[:, hh * S:(hh + 1) * S], -1e30)
                    e = jnp.exp(sh - jnp.max(sh, axis=0, keepdims=True))
                    ps.append((e * (1.0 / jnp.sum(e, axis=0, keepdims=True))).astype(BF16))
                o = dot_nn(v_scr[slot, c * hd:(c + 1) * hd, cols], jnp.concatenate(ps, axis=1))
                o = jnp.concatenate([o[:, hh * S:(hh + 1) * S] for hh in range(nq)], axis=0)
                attn[pl.ds(pl.multiple_of(i * M + t * S, S), S),
                     pl.ds(pl.multiple_of((p * CORES + c) * qw, qw), qw)] = o.T.astype(BF16)

    finish(plan_w[0], wsem.at[0])
    produce(0, 0)

    @pl.loop(0, chips * steps)
    def _(it):
        nxt = jnp.minimum(it + 1, chips * steps - 1)
        for p in range(1, chips):
            @pl.when(it == p * steps - 1)
            def _():
                finish(plan_w[p], wsem.at[p])
        consume(it, it % 2)
        produce(nxt, (it + 1) % 2)

    start(plan_o, wsem.at[chips])
    o_base = n_dev * qw + n_ad * rank
    o_slots = 3

    def o_copies(i, slot):
        return [pltpu.make_async_copy(h.at[pl.ds(pl.multiple_of(o_base + slot * M + t * S, S), S)],
                                      out_ref.at[t, i], osem.at[slot]) for t in range(chips)]

    for c in x_copies(0, h, o_base, 0):
        c.start()
    finish(plan_o, wsem.at[chips])
    nt = 256

    @pl.loop(0, steps)
    def _(i):
        slot = i % o_slots
        nslot = (i + 1) % o_slots
        for c in x_copies(i, h, o_base, slot):
            c.wait()

        @pl.when(i + 1 < steps)
        def _():
            @pl.when(i + 1 >= o_slots)
            def _():
                for c in o_copies(i + 1 - o_slots, nslot):
                    c.wait()
            for c in x_copies(i + 1, h, o_base, nslot):
                c.start()

        for t in range(chips):
            rows = pl.ds(pl.multiple_of(i * M + t * S, S), S)
            a = low[pl.ds(pl.multiple_of(seq_id(i, t) * n_dev * qw, qw), n_dev * qw), :rank]
            lowo[pl.ds(t * S, S), :] = dot_nn(attn[rows, :], a).astype(BF16)

        @pl.loop(0, D // nt)
        def _(j):
            cols = pl.ds(pl.multiple_of(j * nt, nt), nt)
            zo = dot_nn(attn[tile(i), :], h[pl.ds(0, n_dev * qw), cols])
            for t in range(chips):
                b = h[pl.ds(pl.multiple_of(n_dev * qw + seq_id(i, t) * rank, rank), rank), cols]
                z = zo[t * S:(t + 1) * S] + scale * dot_nn(lowo[pl.ds(t * S, S), :], b)
                rows = pl.ds(pl.multiple_of(o_base + slot * M + t * S, S), S)
                h[rows, cols] = (h[rows, cols].astype(F32) + z).astype(BF16)
        for c in o_copies(i, slot):
            c.start()

    for i in range(max(0, steps - o_slots), steps):
        for c in o_copies(i, i % o_slots):
            c.wait()


def mlp_body(dims, meta, x_ref, gain_ref, agu_ref, wg0, wg1, wu0, wu1, wd0, wd1, bg0, bg1, bu0, bu1, ad0, ad1,
             out_ref, wg, wu, wd, bg, bu, agu, ad, h_scr, low_scr, hid_scr, sems):
    seqs, S, rank, D, spc, base_step, chips = dims
    scale = ALPHA / rank
    step = pl.program_id(0)
    core = meta[meta.shape[0] - 1]
    fw = wg0.shape[1]
    plans = [[(agu_ref, agu)], [], []]
    for i, (g, u, b1, b2) in enumerate(((wg0, wu0, bg0, bu0), (wg1, wu1, bg1, bu1))):
        c = pl.ds(i * fw, fw)
        plans[1] += [(g, wg.at[:, c]), (u, wu.at[:, c]), (b1, bg.at[:, :, c]), (b2, bu.at[:, :, c])]
    for i, (d, a) in enumerate(((wd0, ad0), (wd1, ad1))):
        c = pl.ds(i * fw, fw)
        plans[2] += [(a, ad.at[:, c]), (d, wd.at[c])]

    @pl.when(step == 0)
    def _():
        for i, plan in enumerate(plans):
            for src, dst in plan:
                pltpu.make_async_copy(src, dst, sems.at[i]).start()

    def arrive(i):
        @pl.when(step == 0)
        def _():
            for src, dst in plans[i]:
                pltpu.make_async_copy(src, dst, sems.at[i]).wait()

    per = seqs // chips
    ids = [meta[t * per + core * (per // CORES) + base_step + step] for t in range(chips)]
    M = chips * S

    def load_x(i, n):
        t = i // (S // n)
        r = i % (S // n)
        return x_ref[t, 0, pl.ds(pl.multiple_of(r * n, n), n), :]

    norm_tile(load_x, gain_ref, h_scr, M)
    arrive(0)
    for t in range(chips):
        low_scr[pl.ds(t * S, S), :] = dot_nn(h_scr[pl.ds(t * S, S), :], agu[ids[t]]).astype(BF16)
    arrive(1)
    nt = 256

    @pl.loop(0, wg.shape[1] // nt)
    def _(j):
        cols = pl.ds(pl.multiple_of(j * nt, nt), nt)
        zg = dot_nn(h_scr[...], wg[:, cols])
        zu = dot_nn(h_scr[...], wu[:, cols])
        for t in range(chips):
            rows = pl.ds(t * S, S)
            g = zg[t * S:(t + 1) * S] + scale * dot_nn(low_scr[rows, :rank], bg[ids[t], :, cols])
            u = zu[t * S:(t + 1) * S] + scale * dot_nn(low_scr[rows, rank:], bu[ids[t], :, cols])
            hid_scr[rows, cols] = (jax.nn.silu(g) * u).astype(BF16)

    arrive(2)
    for t in range(chips):
        out_ref[t, :, D:] = dot_nn(hid_scr[pl.ds(t * S, S), :], ad[ids[t]]).astype(BF16)

    @pl.loop(0, D // nt)
    def _(j):
        cols = pl.ds(pl.multiple_of(j * nt, nt), nt)
        z = dot_nn(hid_scr[...], wd[:, cols])
        for t in range(chips):
            out_ref[t, :, cols] = z[t * S:(t + 1) * S].astype(BF16)


def finish_body(dims, meta, x_ref, rs_ref, bd_ref, out_ref):
    rank, D = dims
    scale = ALPHA / rank
    nt = 256
    low = rs_ref[0, :, D:]

    @pl.loop(0, D // nt)
    def _(j):
        cols = pl.ds(pl.multiple_of(j * nt, nt), nt)
        delta = scale * dot_nn(low, bd_ref[0, :, cols])
        out_ref[0, :, cols] = (x_ref[0, 0, :, cols].astype(F32) + rs_ref[0, :, cols].astype(F32) + delta).astype(BF16)


def solution(mesh):
    n_dev = mesh.shape['tensor']
    chips = n_dev // CORES
    head_split = P(None, 'tensor', None)
    last_split = P(None, None, 'tensor')
    b_head_split = P(None, None, 'tensor', None)
    in_specs = (P('data', None, None), P('data'), P(None), P(None),
                head_split, head_split, head_split, P('tensor', None, None),
                P(None, 'tensor'), P(None, 'tensor'), P('tensor', None),
                last_split, b_head_split, last_split, b_head_split, last_split, b_head_split,
                P(None, 'tensor', None, None), last_split,
                last_split, last_split, last_split, last_split,
                P(None, 'tensor', None), last_split)
    same_core = [[c + CORES * i for i in range(chips)] for c in range(CORES)]
    swap = [(i, i ^ 1) for i in range(n_dev)]
    ANY = pl.BlockSpec(memory_space=pl.ANY)

    def local_layer(x_in, adapter_ids, gain_attn, gain_mlp, w_q, w_k, w_v, w_o, w_gate, w_up, w_down, a_q, b_q, a_k, b_k, a_v, b_v, a_o, b_o, a_gate, b_gate, a_up, b_up, a_down, b_down):
        seqs, S, D = x_in.shape
        nq, hd = w_q.shape[1], w_q.shape[2]
        n_ad, rank = b_q.shape[0], b_q.shape[1]
        rl = a_q.shape[2]
        half = hd // 2
        qw = nq * hd
        me = lax.axis_index('tensor')
        core, chip = me % CORES, me // CORES
        meta = jnp.concatenate([adapter_ids.astype(jnp.int32), core.reshape(1).astype(jnp.int32)])
        per = seqs // chips
        steps = per // CORES
        spc = steps // CHUNKS

        def rows_t(w):
            return jnp.transpose(w, (1, 2, 0)).reshape(-1, w.shape[0])

        gather = functools.partial(lax.all_gather, axis_name='tensor', axis=0)
        swapped = functools.partial(lax.ppermute, axis_name='tensor', perm=swap)

        g_a = gather(jnp.concatenate([jnp.transpose(a, (0, 2, 1)).reshape(n_ad * rl, D)
                                      for a in (a_q, a_k, a_v, a_gate, a_up)], axis=0))
        g_a = g_a.reshape(n_dev, 5, n_ad, rl, D)
        a_qkv = g_a[:, :3].transpose(2, 1, 0, 3, 4).reshape(n_ad * 3 * rank, D)
        a_gu = g_a[:, 3:].transpose(2, 4, 1, 0, 3).reshape(n_ad, D, 2 * rank)
        g_w = gather(jnp.concatenate([rows_t(w_q), rows_t(w_k), rows_t(w_v)], axis=0))

        def b_rows(b):
            return jnp.transpose(b, (1, 2, 0)).reshape(-1, rank)

        b_parts = []
        for a in range(n_ad):
            b_parts += [b_rows(b_q[a]), b_rows(b_k[a]), b_rows(b_v[a])]
        b_parts += [a_o.reshape(n_ad * qw, rank), b_o.reshape(n_ad * rank, qw)]
        g_b = gather(jnp.concatenate(b_parts, axis=0))
        g_wo = gather(w_o.reshape(qw, D))
        g_bd = gather(b_down.reshape(n_ad * rank, qw))
        bd_full = g_bd.reshape(n_dev, n_ad, rank, qw).transpose(1, 2, 0, 3).reshape(n_ad, rank, D)
        mlp_own = (w_gate, w_up, w_down, b_gate, b_up, a_down)
        mlp_other = tuple(swapped(w) for w in mlp_own)

        inv_freq = ROPE_BASE ** (-2.0 * jnp.arange(half, dtype=F32) / hd)
        ang = jnp.arange(S, dtype=F32)[:, None] * inv_freq[None, :]
        cos, sin = jnp.cos(ang), jnp.sin(ang)
        cos_t, sin_t = cos.T, sin.T

        x4 = x_in.reshape(chips, per, S, D)
        M = chips * S
        Fc = CORES * w_gate.shape[1]
        full = lambda shape: pl.BlockSpec(shape, lambda i, m: (0,) * len(shape))
        params = pltpu.CompilerParams(vmem_limit_bytes=VMEM_LIMIT, dimension_semantics=("arbitrary",))
        y = jnp.zeros((n_dev, steps * S, D), BF16)
        x1_all = pl.pallas_call(
            functools.partial(attn_body, (n_dev, seqs, S, hd, nq, rank, D, chips)),
            in_specs=[pl.BlockSpec(memory_space=pltpu.SMEM), ANY] + [pl.BlockSpec(memory_space=pltpu.VMEM)] * 3 + [ANY] * 4,
            out_specs=ANY,
            scratch_shapes=[
                pltpu.VMEM((steps * M, D), BF16), pltpu.VMEM((steps * M, 3 * rank), BF16), pltpu.VMEM((steps * M, n_dev * qw), BF16),
                pltpu.VMEM((chips, CORES * (qw + 2 * hd), D), BF16), pltpu.VMEM((chips, n_ad, CORES * (qw + 2 * hd), rank), BF16),
                pltpu.VMEM((2, CORES * qw, M), BF16), pltpu.VMEM((2, CORES, M, hd), BF16), pltpu.VMEM((2, CORES * hd, M), BF16),
                pltpu.VMEM((M, rank), BF16),
                pltpu.SemaphoreType.DMA((chips + 1,)), pltpu.SemaphoreType.DMA((3,)), pltpu.SemaphoreType.DMA((3,))],
            out_shape=jax.ShapeDtypeStruct((chips, steps, S, D), BF16),
            compiler_params=pltpu.CompilerParams(vmem_limit_bytes=VMEM_LIMIT), name="attn_block",
            cost_estimate=pl.CostEstimate(flops=3 * steps * M * D * (2 * n_dev * qw + 2 * n_dev * hd + 4 * rank),
                                          bytes_accessed=6 * steps * M * D + 33 * 2**20, transcendentals=0),
        )(adapter_ids, x4, gain_attn.reshape(1, D), cos_t, sin_t, g_w, a_qkv, g_b, g_wo)
        for c in range(CHUNKS):
            base_step = c * spc
            tok = M * spc
            pairs = [w for own, other in zip(mlp_own, mlp_other) for w in (own, other)]
            part = pl.pallas_call(
                functools.partial(mlp_body, (seqs, S, rank, D, spc, base_step, chips)),
                grid_spec=pltpu.PrefetchScalarGridSpec(
                    num_scalar_prefetch=1, grid=(spc,),
                    in_specs=[pl.BlockSpec((chips, 1, S, D), lambda i, m, b=base_step: (0, b + i, 0, 0)), full((1, D))] + [ANY] * 13,
                    out_specs=pl.BlockSpec((chips, S, D + rank), lambda i, m: (0, i, 0)),
                    scratch_shapes=[
                        pltpu.VMEM((D, Fc), BF16), pltpu.VMEM((D, Fc), BF16), pltpu.VMEM((Fc, D), BF16),
                        pltpu.VMEM((n_ad, rank, Fc), BF16), pltpu.VMEM((n_ad, rank, Fc), BF16),
                        pltpu.VMEM((n_ad, D, 2 * rank), BF16), pltpu.VMEM((n_ad, Fc, rank), BF16),
                        pltpu.VMEM((M, D), BF16), pltpu.VMEM((M, 2 * rank), BF16), pltpu.VMEM((M, Fc), BF16),
                        pltpu.SemaphoreType.DMA((3,))]),
                out_shape=jax.ShapeDtypeStruct((chips, spc * S, D + rank), BF16),
                compiler_params=params, name="mlp_block",
                cost_estimate=pl.CostEstimate(flops=2 * tok * D * (3 * Fc + 4 * rank),
                                              bytes_accessed=4 * tok * D + 34 * 2**20, transcendentals=tok * Fc),
            )(meta, x1_all, gain_mlp.reshape(1, D), a_gu, *pairs)
            rs = lax.psum_scatter(part, 'tensor', scatter_dimension=0, axis_index_groups=same_core, tiled=True)
            own = [adapter_ids[chip * per + core * steps + base_step + i] for i in range(spc)]
            meta2 = jnp.concatenate([jnp.stack(own).astype(jnp.int32), chip.reshape(1).astype(jnp.int32)])
            y_own = pl.pallas_call(
                functools.partial(finish_body, (rank, D)),
                grid_spec=pltpu.PrefetchScalarGridSpec(
                    num_scalar_prefetch=1, grid=(spc,),
                    in_specs=[pl.BlockSpec((1, 1, S, D), lambda i, m, b=base_step: (m[spc], b + i, 0, 0)),
                              pl.BlockSpec((1, S, D + rank), lambda i, m: (i, 0, 0)),
                              pl.BlockSpec((1, rank, D), lambda i, m: (m[i], 0, 0))],
                    out_specs=pl.BlockSpec((1, S, D), lambda i, m: (i, 0, 0))),
                out_shape=jax.ShapeDtypeStruct((spc, S, D), BF16),
                compiler_params=pltpu.CompilerParams(dimension_semantics=("arbitrary",)), name="finish",
                cost_estimate=pl.CostEstimate(flops=2 * spc * S * rank * D, bytes_accessed=10 * spc * S * D, transcendentals=0),
            )(meta2, x1_all, rs.reshape(spc, S, D + rank), bd_full)
            y_all = gather(y_own.reshape(spc * S, D))
            y = lax.dynamic_update_slice(y, y_all, (0, base_step * S, 0))
        return y.reshape(seqs, S, D)

    return jax.shard_map(local_layer, mesh=mesh, in_specs=in_specs, out_specs=P('data', None, None), check_vma=False)
```

```python
import functools

import jax
import jax.numpy as jnp
from jax import lax
from jax.experimental import pallas as pl
from jax.experimental.pallas import tpu as pltpu
from jax.sharding import PartitionSpec as P

ALPHA = 16.0
ROPE_BASE = 10000.0
EPSILON = 1e-5
CORES = 2
VMEM_LIMIT = 62 * 1024 * 1024
F32, BF16 = jnp.float32, jnp.bfloat16


def dot_nn(a, b):
    return lax.dot_general(a, b, (((1,), (0,)), ((), ())), preferred_element_type=F32)


def dot_nt(a, b):
    return lax.dot_general(a, b, (((1,), (1,)), ((), ())), preferred_element_type=F32)


def attn_body(dims, ids_ref, x_ref, gain_ref, cos_ref, sin_ref, gw_ref, aqkv_ref, gb_ref, gwo_ref, out_ref,
              h, low, attn, w, bw, q_scr, k_scr, v_scr, lowo, wsem, xsem, osem):
    n_dev, seqs, S, hd, nq, rank, D, chips = dims
    half = hd // 2
    qw = nq * hd
    n_ad = 2
    scale = ALPHA / rank
    core = lax.axis_index('tensor') % CORES
    per = seqs // chips
    steps = per // CORES
    M = chips * S
    pw = CORES * (qw + 2 * hd)
    kw = CORES * qw
    vw = kw + CORES * hd

    def seq_id(i, t):
        return ids_ref[t * per + core * steps + i]

    def tile(i):
        return pl.ds(pl.multiple_of(i * M, M), M)

    a_rows = n_ad * 3 * rank
    x_base = 4 * M
    plan_a = [(aqkv_ref, attn.at[pl.ds(0, a_rows)])]
    plan_w = []
    for p in range(chips):
        plan = []
        for c in range(CORES):
            d = p * CORES + c
            plan += [(gw_ref.at[d, pl.ds(0, qw)], w.at[p, pl.ds(c * qw, qw)]),
                     (gw_ref.at[d, pl.ds(qw, hd)], w.at[p, pl.ds(kw + c * hd, hd)]),
                     (gw_ref.at[d, pl.ds(qw + hd, hd)], w.at[p, pl.ds(vw + c * hd, hd)])]
            for a in range(n_ad):
                o = a * (qw + 2 * hd)
                plan += [(gb_ref.at[d, pl.ds(o, qw)], bw.at[p, a, pl.ds(c * qw, qw)]),
                         (gb_ref.at[d, pl.ds(o + qw, hd)], bw.at[p, a, pl.ds(kw + c * hd, hd)]),
                         (gb_ref.at[d, pl.ds(o + qw + hd, hd)], bw.at[p, a, pl.ds(vw + c * hd, hd)])]
        plan_w.append(plan)
    plan_o = []
    off = n_ad * (qw + 2 * hd)
    for d in range(n_dev):
        plan_o.append((gwo_ref.at[d], h.at[pl.ds(d * qw, qw)]))
        for a in range(n_ad):
            plan_o.append((gb_ref.at[d, pl.ds(off + a * qw, qw)], low.at[pl.ds((a * n_dev + d) * qw, qw), pl.ds(0, rank)]))
            plan_o.append((gb_ref.at[d, pl.ds(off + n_ad * qw + a * rank, rank)],
                           h.at[pl.ds(n_dev * qw + a * rank, rank), pl.ds(d * qw, qw)]))

    def start(plan, sem):
        for s, d in plan:
            pltpu.make_async_copy(s, d, sem).start()

    def finish(plan, sem):
        for s, d in plan:
            pltpu.make_async_copy(s, d, sem).wait()

    def x_copies(i, buf, base, slot):
        return [pltpu.make_async_copy(x_ref.at[t, core * steps + i],
                                      buf.at[pl.ds(pl.multiple_of(base + slot * M + t * S, S), S)], xsem.at[slot])
                for t in range(chips)]

    start(plan_a, wsem.at[chips])
    for c in x_copies(0, attn, x_base, 0):
        c.start()
    for p in range(chips):
        start(plan_w[p], wsem.at[p])

    rb = 16

    @pl.loop(0, steps)
    def _(i):
        slot = i % 2
        for c in x_copies(i, attn, x_base, slot):
            c.wait()

        @pl.when(i + 1 < steps)
        def _():
            for c in x_copies(i + 1, attn, x_base, 1 - slot):
                c.start()

        @pl.loop(0, M // rb)
        def _(r):
            v = attn[pl.ds(pl.multiple_of(x_base + slot * M + r * rb, rb), rb), :].astype(F32)
            inv = lax.rsqrt(jnp.mean(v * v, axis=-1, keepdims=True) + EPSILON)
            h[pl.ds(pl.multiple_of(i * M + r * rb, rb), rb), :] = (v * inv * gain_ref[...]).astype(BF16)

        @pl.when(i == 0)
        def _():
            finish(plan_a, wsem.at[chips])
        for t in range(chips):
            rows = pl.ds(pl.multiple_of(i * M + t * S, S), S)
            a = attn[pl.ds(pl.multiple_of(seq_id(i, t) * 3 * rank, 3 * rank), 3 * rank), :]
            low[rows, :] = dot_nt(h[rows, :], a).astype(BF16)

    def produce(it, slot):
        p, i = it // steps, it % steps
        z = dot_nt(w[p], h[tile(i), :])
        for t in range(chips):
            rows = pl.ds(pl.multiple_of(i * M + t * S, S), S)
            b = bw[p, seq_id(i, t)]
            lo = low[rows, :]
            cols = slice(t * S, (t + 1) * S)
            zq = z[:kw, cols] + scale * dot_nt(b[:kw], lo[:, :rank])
            zk = z[kw:vw, cols] + scale * dot_nt(b[kw:vw], lo[:, rank:2 * rank])
            zv = z[vw:, cols] + scale * dot_nt(b[vw:], lo[:, 2 * rank:])
            cos, sin = cos_ref[...], sin_ref[...]

            def rotate(v):
                f, s = v[:half], v[half:]
                return jnp.concatenate([f * cos - s * sin, s * cos + f * sin], axis=0)

            for hh in range(CORES * nq):
                o = hh * hd
                q_scr[slot, o:o + hd, cols] = (rotate(zq[o:o + hd]) * hd ** -0.5).astype(BF16)
            kt = jnp.concatenate([rotate(zk[c * hd:(c + 1) * hd]) for c in range(CORES)], axis=0)
            kk = kt.T.astype(BF16)
            for c in range(CORES):
                k_scr[slot, c, t * S:(t + 1) * S, :] = kk[:, c * hd:(c + 1) * hd]
            v_scr[slot, :, cols] = zv.astype(BF16)

    def consume(it, slot):
        p, i = it // steps, it % steps
        key = lax.broadcasted_iota(jnp.int32, (S, S), 0)
        qry = lax.broadcasted_iota(jnp.int32, (S, S), 1)
        causal = key <= qry
        for c in range(CORES):
            for t in range(chips):
                cols = slice(t * S, (t + 1) * S)
                q = jnp.concatenate([q_scr[slot, c * qw + hh * hd:c * qw + (hh + 1) * hd, cols] for hh in range(nq)], axis=1)
                sc = dot_nn(k_scr[slot, c, cols, :], q)
                ps = []
                for hh in range(nq):
                    sh = jnp.where(causal, sc[:, hh * S:(hh + 1) * S], -1e30)
                    e = jnp.exp(sh - jnp.max(sh, axis=0, keepdims=True))
                    ps.append((e * (1.0 / jnp.sum(e, axis=0, keepdims=True))).astype(BF16))
                o = dot_nn(v_scr[slot, c * hd:(c + 1) * hd, cols], jnp.concatenate(ps, axis=1))
                o = jnp.concatenate([o[:, hh * S:(hh + 1) * S] for hh in range(nq)], axis=0)
                attn[pl.ds(pl.multiple_of(i * M + t * S, S), S),
                     pl.ds(pl.multiple_of((p * CORES + c) * qw, qw), qw)] = o.T.astype(BF16)

    finish(plan_w[0], wsem.at[0])
    produce(0, 0)

    @pl.loop(0, chips * steps)
    def _(it):
        nxt = jnp.minimum(it + 1, chips * steps - 1)
        for p in range(1, chips):
            @pl.when(it == p * steps - 1)
            def _():
                finish(plan_w[p], wsem.at[p])
        consume(it, it % 2)
        produce(nxt, (it + 1) % 2)

    start(plan_o, wsem.at[chips])
    o_base = n_dev * qw + n_ad * rank
    o_slots = 3

    def o_copies(i, slot):
        return [pltpu.make_async_copy(h.at[pl.ds(pl.multiple_of(o_base + slot * M + t * S, S), S)],
                                      out_ref.at[t, i], osem.at[slot]) for t in range(chips)]

    for c in x_copies(0, h, o_base, 0):
        c.start()
    finish(plan_o, wsem.at[chips])
    nt = 256

    @pl.loop(0, steps)
    def _(i):
        slot = i % o_slots
        nslot = (i + 1) % o_slots
        for c in x_copies(i, h, o_base, slot):
            c.wait()

        @pl.when(i + 1 < steps)
        def _():
            @pl.when(i + 1 >= o_slots)
            def _():
                for c in o_copies(i + 1 - o_slots, nslot):
                    c.wait()
            for c in x_copies(i + 1, h, o_base, nslot):
                c.start()

        for t in range(chips):
            rows = pl.ds(pl.multiple_of(i * M + t * S, S), S)
            a = low[pl.ds(pl.multiple_of(seq_id(i, t) * n_dev * qw, qw), n_dev * qw), :rank]
            lowo[pl.ds(t * S, S), :] = dot_nn(attn[rows, :], a).astype(BF16)

        @pl.loop(0, D // nt)
        def _(j):
            cols = pl.ds(pl.multiple_of(j * nt, nt), nt)
            zo = dot_nn(attn[tile(i), :], h[pl.ds(0, n_dev * qw), cols])
            for t in range(chips):
                b = h[pl.ds(pl.multiple_of(n_dev * qw + seq_id(i, t) * rank, rank), rank), cols]
                z = zo[t * S:(t + 1) * S] + scale * dot_nn(lowo[pl.ds(t * S, S), :], b)
                rows = pl.ds(pl.multiple_of(o_base + slot * M + t * S, S), S)
                h[rows, cols] = (h[rows, cols].astype(F32) + z).astype(BF16)
        for c in o_copies(i, slot):
            c.start()

    for i in range(max(0, steps - o_slots), steps):
        for c in o_copies(i, i % o_slots):
            c.wait()


def mlp_body(dims, ids_ref, x_ref, gain_ref, agu_ref, wg0, wg1, wu0, wu1, wd0, wd1, bg0, bg1, bu0, bu1, ad0, ad1, bd_ref,
             y_ref, wg, wu, wd, bg, bu, agu, ad, bd, xt, h_scr, low_scr, hid_scr, part, in_a, in_b, xo, ybuf,
             wsem, xsem, osem, sa, ra, sb, rb_, sy, ry, sf, rf, sp, rp):
    seqs, S, rank, D, chips = dims
    scale = ALPHA / rank
    fw = wg0.shape[1]
    per = seqs // chips
    steps = per // CORES
    M = chips * S
    hs = S // 2
    me = lax.axis_index('tensor')
    core, chip = me % CORES, me // CORES
    right_chip, left_chip = (chip + 1) % chips, (chip + chips - 1) % chips
    far_chip = (chip + 2) % chips
    right, left, other = right_chip * CORES + core, left_chip * CORES + core, chip * CORES + (1 - core)

    barrier = pltpu.get_barrier_semaphore()
    for dev in (right, left, other):
        pl.semaphore_signal(barrier, inc=1, device_id={'tensor': dev}, device_id_type=pl.DeviceIdType.MESH)
    pl.semaphore_wait(barrier, 3)

    def remote(src, dst, ssem, rsem, dev):
        return pltpu.make_async_remote_copy(src_ref=src, dst_ref=dst, send_sem=ssem, recv_sem=rsem,
                                            device_id={'tensor': dev}, device_id_type=pl.DeviceIdType.MESH)

    def copies_a(j):
        s, r = j % 3, j % 4
        return [remote(part.at[s, far_chip, pl.ds(0, hs)], in_a.at[0, r], sa.at[0, j], ra.at[0, j], right),
                remote(part.at[s, far_chip, pl.ds(hs, hs)], in_a.at[1, r], sa.at[1, j], ra.at[1, j], left)]

    def copies_b(j):
        s, r = j % 3, j % 3
        return [remote(part.at[s, right_chip], in_b.at[0, r], sb.at[0, j], rb_.at[0, j], right),
                remote(part.at[s, left_chip], in_b.at[1, r], sb.at[1, j], rb_.at[1, j], left)]

    def copies_y(j):
        dst = y_ref.at[me, j]
        src = ybuf.at[j % 2]
        return [remote(src, dst, sy.at[0, j], ry.at[0, j], right), remote(src, dst, sy.at[1, j], ry.at[1, j], left)]

    def copies_f(j):
        from_left = y_ref.at[left, j, pl.ds(0, hs)]
        from_right = y_ref.at[right, j, pl.ds(hs, hs)]
        return [remote(from_left, from_left, sf.at[0, j], rf.at[0, j], right),
                remote(from_right, from_right, sf.at[1, j], rf.at[1, j], left)]

    far = far_chip * CORES + core

    def copies_p(j):
        out = [remote(ybuf.at[j % 2], y_ref.at[me, j], sp.at[0, j], rp.at[0, j], other)]
        for n, dev in enumerate((left, right, far)):
            out.append(remote(y_ref.at[dev, j], y_ref.at[dev, j], sp.at[n + 1, j], rp.at[n + 1, j], other))
        return out

    def store_y(j):
        return pltpu.make_async_copy(ybuf.at[j % 2], y_ref.at[me, j], osem.at[j % 2])

    plans = [[(agu_ref, agu)], [], [(bd_ref, bd)]]
    for i, (g, u, b1, b2) in enumerate(((wg0, wu0, bg0, bu0), (wg1, wu1, bg1, bu1))):
        c = pl.ds(i * fw, fw)
        plans[1] += [(g, wg.at[:, c]), (u, wu.at[:, c]), (b1, bg.at[:, :, c]), (b2, bu.at[:, :, c])]
    for i, (d, a) in enumerate(((wd0, ad0), (wd1, ad1))):
        c = pl.ds(i * fw, fw)
        plans[2] += [(a, ad.at[:, c]), (d, wd.at[c])]
    n_plan = [0]
    flat = []
    for plan in plans:
        group = []
        for src, dst in plan:
            group.append(pltpu.make_async_copy(src, dst, wsem.at[n_plan[0]]))
            n_plan[0] += 1
        flat.append(group)

    def x_copy(i, slot):
        return pltpu.make_async_copy(x_ref.at[:, i], xt.at[slot], xsem.at[slot])

    def xo_copy(i):
        return pltpu.make_async_copy(x_ref.at[chip, i], xo.at[i % 2], xsem.at[2 + i % 2])

    x_copy(0, 0).start()
    for group in flat:
        for c in group:
            c.start()

    def arrive(i, step):
        @pl.when(step == 0)
        def _():
            for c in flat[i]:
                c.wait()

    nt = 256
    rb = 16

    def compute(k):
        slot = k % 2
        x_copy(k, slot).wait()

        @pl.when(k + 1 < steps)
        def _():
            x_copy(k + 1, 1 - slot).start()

        ids = [ids_ref[t * per + core * steps + k] for t in range(chips)]

        @pl.loop(0, M // rb)
        def _(i):
            t, r = i // (S // rb), i % (S // rb)
            v = xt[slot, t, pl.ds(pl.multiple_of(r * rb, rb), rb), :].astype(F32)
            inv = lax.rsqrt(jnp.mean(v * v, axis=-1, keepdims=True) + EPSILON)
            h_scr[pl.ds(pl.multiple_of(i * rb, rb), rb), :] = (v * inv * gain_ref[...]).astype(BF16)

        arrive(0, k)
        for t in range(chips):
            low_scr[pl.ds(t * S, S), :] = dot_nn(h_scr[pl.ds(t * S, S), :], agu[ids[t]]).astype(BF16)
        arrive(1, k)

        @pl.loop(0, wg.shape[1] // nt)
        def _(j):
            cols = pl.ds(pl.multiple_of(j * nt, nt), nt)
            zg = dot_nn(h_scr[...], wg[:, cols])
            zu = dot_nn(h_scr[...], wu[:, cols])
            for t in range(chips):
                rows = pl.ds(t * S, S)
                g = zg[t * S:(t + 1) * S] + scale * dot_nn(low_scr[rows, :rank], bg[ids[t], :, cols])
                u = zu[t * S:(t + 1) * S] + scale * dot_nn(low_scr[rows, rank:], bu[ids[t], :, cols])
                hid_scr[rows, cols] = (jax.nn.silu(g) * u).astype(BF16)

        arrive(2, k)

        @pl.when(k >= 3)
        def _():
            for c in copies_a(k - 3) + copies_b(k - 3):
                c.wait_send()
        s = k % 3
        for t in range(chips):
            part[s, t, :, D:] = dot_nn(hid_scr[pl.ds(t * S, S), :], ad[ids[t]]).astype(BF16)

        @pl.loop(0, D // nt)
        def _(j):
            cols = pl.ds(pl.multiple_of(j * nt, nt), nt)
            z = dot_nn(hid_scr[...], wd[:, cols])
            for t in range(chips):
                part[s, t, :, cols] = z[t * S:(t + 1) * S].astype(BF16)

        for c in copies_a(k):
            c.start()

    def relay(j):
        s, r = j % 3, j % 4
        for n, (dest, lo) in enumerate(((right_chip, 0), (left_chip, hs))):
            copies_a(j)[n].wait_recv()

            @pl.loop(0, hs // rb)
            def _(i):
                rows = pl.ds(pl.multiple_of(lo + i * rb, rb), rb)
                got = in_a[n, r, pl.ds(pl.multiple_of(i * rb, rb), rb), :]
                part[s, dest, rows, :] = (part[s, dest, rows, :].astype(F32) + got.astype(F32)).astype(BF16)
            copies_b(j)[n].start()
        xo_copy(j).start()

    def settle(j):
        s = j % 3
        for c in copies_b(j):
            c.wait_recv()
        xo_copy(j).wait()

        @pl.when(j >= 2)
        def _():
            store_y(j - 2).wait()
            for c in copies_y(j - 2) + copies_p(j - 2)[:1]:
                c.wait_send()
        idx = ids_ref[chip * per + core * steps + j]

        def total(cols):
            return (part[s, chip, :, cols].astype(F32) + in_b[0, s, :, cols].astype(F32)) + in_b[1, s, :, cols].astype(F32)

        low = total(pl.ds(D, rank)).astype(BF16)

        @pl.loop(0, D // nt)
        def _(i):
            cols = pl.ds(pl.multiple_of(i * nt, nt), nt)
            z = total(cols) + scale * dot_nn(low, bd[idx, :, cols])
            ybuf[j % 2, :, cols] = (xo[j % 2, :, cols].astype(F32) + z).astype(BF16)
        store_y(j).start()
        for c in copies_y(j) + copies_p(j)[:1]:
            c.start()

    def forward(j):
        for n in range(2):
            copies_y(j)[n].wait_recv()
            copies_f(j)[n].start()
            copies_p(j)[1 + n].start()

    def last_hop(j):
        for c in copies_f(j):
            c.wait_recv()
        copies_p(j)[3].start()

    @pl.loop(0, steps + 4)
    def _(k):
        @pl.when(k < steps)
        def _():
            compute(k)
        for lag, stage in ((1, relay), (2, settle), (3, forward), (4, last_hop)):
            @pl.when((k >= lag) & (k < steps + lag))
            def _():
                stage(k - lag)

    for j in range(max(0, steps - 3), steps):
        for c in copies_a(j) + copies_b(j):
            c.wait_send()
    for j in range(max(0, steps - 2), steps):
        store_y(j).wait()
        for c in copies_y(j) + copies_p(j)[:1]:
            c.wait_send()

    @pl.loop(0, steps)
    def _(j):
        for c in copies_f(j) + copies_p(j)[1:]:
            c.wait_send()
        for c in copies_p(j):
            c.wait_recv()


def solution(mesh):
    n_dev = mesh.shape['tensor']
    chips = n_dev // CORES
    head_split = P(None, 'tensor', None)
    last_split = P(None, None, 'tensor')
    b_head_split = P(None, None, 'tensor', None)
    in_specs = (P('data', None, None), P('data'), P(None), P(None),
                head_split, head_split, head_split, P('tensor', None, None),
                P(None, 'tensor'), P(None, 'tensor'), P('tensor', None),
                last_split, b_head_split, last_split, b_head_split, last_split, b_head_split,
                P(None, 'tensor', None, None), last_split,
                last_split, last_split, last_split, last_split,
                P(None, 'tensor', None), last_split)
    swap = [(i, i ^ 1) for i in range(n_dev)]
    ANY = pl.BlockSpec(memory_space=pl.ANY)

    def local_layer(x_in, adapter_ids, gain_attn, gain_mlp, w_q, w_k, w_v, w_o, w_gate, w_up, w_down, a_q, b_q, a_k, b_k, a_v, b_v, a_o, b_o, a_gate, b_gate, a_up, b_up, a_down, b_down):
        seqs, S, D = x_in.shape
        nq, hd = w_q.shape[1], w_q.shape[2]
        n_ad, rank = b_q.shape[0], b_q.shape[1]
        rl = a_q.shape[2]
        half = hd // 2
        qw = nq * hd
        per = seqs // chips
        steps = per // CORES

        def rows_t(w):
            return jnp.transpose(w, (1, 2, 0)).reshape(-1, w.shape[0])

        gather = functools.partial(lax.all_gather, axis_name='tensor', axis=0)
        swapped = functools.partial(lax.ppermute, axis_name='tensor', perm=swap)

        g_a = gather(jnp.concatenate([jnp.transpose(a, (0, 2, 1)).reshape(n_ad * rl, D)
                                      for a in (a_q, a_k, a_v, a_gate, a_up)], axis=0))
        g_a = g_a.reshape(n_dev, 5, n_ad, rl, D)
        a_qkv = g_a[:, :3].transpose(2, 1, 0, 3, 4).reshape(n_ad * 3 * rank, D)
        a_gu = g_a[:, 3:].transpose(2, 4, 1, 0, 3).reshape(n_ad, D, 2 * rank)
        g_w = gather(jnp.concatenate([rows_t(w_q), rows_t(w_k), rows_t(w_v)], axis=0))

        def b_rows(b):
            return jnp.transpose(b, (1, 2, 0)).reshape(-1, rank)

        b_parts = []
        for a in range(n_ad):
            b_parts += [b_rows(b_q[a]), b_rows(b_k[a]), b_rows(b_v[a])]
        b_parts += [a_o.reshape(n_ad * qw, rank), b_o.reshape(n_ad * rank, qw)]
        g_b = gather(jnp.concatenate(b_parts, axis=0))
        g_wo = gather(w_o.reshape(qw, D))
        g_bd = gather(b_down.reshape(n_ad * rank, qw))
        bd_full = g_bd.reshape(n_dev, n_ad, rank, qw).transpose(1, 2, 0, 3).reshape(n_ad, rank, D)
        mlp_own = (w_gate, w_up, w_down, b_gate, b_up, a_down)
        mlp_other = tuple(swapped(w) for w in mlp_own)

        inv_freq = ROPE_BASE ** (-2.0 * jnp.arange(half, dtype=F32) / hd)
        ang = jnp.arange(S, dtype=F32)[:, None] * inv_freq[None, :]
        cos, sin = jnp.cos(ang), jnp.sin(ang)
        cos_t, sin_t = cos.T, sin.T

        x4 = x_in.reshape(chips, per, S, D)
        M = chips * S
        Fc = CORES * w_gate.shape[1]
        x1_all = pl.pallas_call(
            functools.partial(attn_body, (n_dev, seqs, S, hd, nq, rank, D, chips)),
            in_specs=[pl.BlockSpec(memory_space=pltpu.SMEM), ANY] + [pl.BlockSpec(memory_space=pltpu.VMEM)] * 3 + [ANY] * 4,
            out_specs=ANY,
            scratch_shapes=[
                pltpu.VMEM((steps * M, D), BF16), pltpu.VMEM((steps * M, 3 * rank), BF16), pltpu.VMEM((steps * M, n_dev * qw), BF16),
                pltpu.VMEM((chips, CORES * (qw + 2 * hd), D), BF16), pltpu.VMEM((chips, n_ad, CORES * (qw + 2 * hd), rank), BF16),
                pltpu.VMEM((2, CORES * qw, M), BF16), pltpu.VMEM((2, CORES, M, hd), BF16), pltpu.VMEM((2, CORES * hd, M), BF16),
                pltpu.VMEM((M, rank), BF16),
                pltpu.SemaphoreType.DMA((chips + 1,)), pltpu.SemaphoreType.DMA((3,)), pltpu.SemaphoreType.DMA((3,))],
            out_shape=jax.ShapeDtypeStruct((chips, steps, S, D), BF16),
            compiler_params=pltpu.CompilerParams(vmem_limit_bytes=VMEM_LIMIT), name="attn_block",
            cost_estimate=pl.CostEstimate(flops=3 * steps * M * D * (2 * n_dev * qw + 2 * n_dev * hd + 4 * rank),
                                          bytes_accessed=6 * steps * M * D + 33 * 2**20, transcendentals=0),
        )(adapter_ids, x4, gain_attn.reshape(1, D), cos_t, sin_t, g_w, a_qkv, g_b, g_wo)
        pairs = [w for own, other in zip(mlp_own, mlp_other) for w in (own, other)]
        dma = pltpu.SemaphoreType.DMA
        y = pl.pallas_call(
            functools.partial(mlp_body, (seqs, S, rank, D, chips)),
            in_specs=[pl.BlockSpec(memory_space=pltpu.SMEM), ANY, pl.BlockSpec(memory_space=pltpu.VMEM)] + [ANY] * 14,
            out_specs=ANY,
            scratch_shapes=[
                pltpu.VMEM((D, Fc), BF16), pltpu.VMEM((D, Fc), BF16), pltpu.VMEM((Fc, D), BF16),
                pltpu.VMEM((n_ad, rank, Fc), BF16), pltpu.VMEM((n_ad, rank, Fc), BF16),
                pltpu.VMEM((n_ad, D, 2 * rank), BF16), pltpu.VMEM((n_ad, Fc, rank), BF16), pltpu.VMEM((n_ad, rank, D), BF16),
                pltpu.VMEM((2, chips, S, D), BF16), pltpu.VMEM((M, D), BF16), pltpu.VMEM((M, 2 * rank), BF16), pltpu.VMEM((M, Fc), BF16),
                pltpu.VMEM((3, chips, S, D + rank), BF16), pltpu.VMEM((2, 4, S // 2, D + rank), BF16),
                pltpu.VMEM((2, 3, S, D + rank), BF16), pltpu.VMEM((2, S, D), BF16), pltpu.VMEM((2, S, D), BF16),
                dma((14,)), dma((4,)), dma((2,)), dma((2, steps)), dma((2, steps)), dma((2, steps)), dma((2, steps)),
                dma((2, steps)), dma((2, steps)), dma((2, steps)), dma((2, steps)), dma((4, steps)), dma((4, steps))],
            out_shape=jax.ShapeDtypeStruct((n_dev, steps, S, D), BF16),
            compiler_params=pltpu.CompilerParams(vmem_limit_bytes=VMEM_LIMIT, collective_id=0, has_side_effects=True),
            name="mlp_ring",
            cost_estimate=pl.CostEstimate(flops=2 * steps * M * D * (3 * Fc + 4 * rank),
                                          bytes_accessed=8 * steps * M * D + 34 * 2**20, transcendentals=steps * M * Fc),
        )(adapter_ids, x1_all, gain_mlp.reshape(1, D), a_gu, *pairs, bd_full)
        return y.reshape(seqs, S, D)

    return jax.shard_map(local_layer, mesh=mesh, in_specs=in_specs, out_specs=P('data', None, None), check_vma=False)
```

```python
import functools

import jax
import jax.numpy as jnp
from jax import lax
from jax.experimental import pallas as pl
from jax.experimental.pallas import tpu as pltpu
from jax.sharding import PartitionSpec as P

ALPHA = 16.0
ROPE_BASE = 10000.0
EPSILON = 1e-5
CORES = 2
VMEM_LIMIT = 62 * 1024 * 1024
F32, BF16 = jnp.float32, jnp.bfloat16


def dot_nn(a, b):
    return lax.dot_general(a, b, (((1,), (0,)), ((), ())), preferred_element_type=F32)


def dot_nt(a, b):
    return lax.dot_general(a, b, (((1,), (1,)), ((), ())), preferred_element_type=F32)


def attn_body(dims, ids_ref, x_ref, gain_ref, cos_ref, sin_ref, a_own, w_own, b_own, out_ref, ga, gw, gb,
              h, low, attn, w, bw, q_scr, k_scr, v_scr, asem, wsem, xsem, osem, ss, rs):
    n_dev, seqs, S, hd, nq, rank, D, chips = dims
    half = hd // 2
    qw = nq * hd
    n_ad = 2
    scale = ALPHA / rank
    me = lax.axis_index('tensor')
    core, chip = me % CORES, me // CORES
    per = seqs // chips
    steps = per // CORES
    M = chips * S
    dw = qw + 2 * hd
    rl = rank // n_dev
    right_chip, left_chip, far_chip = (chip + 1) % chips, (chip + chips - 1) % chips, (chip + 2) % chips
    order = [(chip + r) % chips for r in range(chips)]
    right, left, far = [c * CORES + core for c in (right_chip, left_chip, far_chip)]
    other = chip * CORES + (1 - core)

    barrier = pltpu.get_barrier_semaphore()
    for dev in (right, left, other):
        pl.semaphore_signal(barrier, inc=1, device_id={'tensor': dev}, device_id_type=pl.DeviceIdType.MESH)
    pl.semaphore_wait(barrier, 3)

    groups = ((a_own, ga), (w_own, gw), (b_own, gb))

    def remote(m, n, src, dst, dev):
        return pltpu.make_async_remote_copy(src_ref=src, dst_ref=dst, send_sem=ss.at[m, n], recv_sem=rs.at[m, n],
                                            device_id={'tensor': dev}, device_id_type=pl.DeviceIdType.MESH)

    def copy(m, n):
        own, buf = groups[m]
        n_rows = own.shape[0] // 2
        if n == 0:
            return remote(m, n, own, buf.at[me], right)
        if n == 1:
            return remote(m, n, own, buf.at[me], left)
        if n == 2:
            part = buf.at[left, pl.ds(0, n_rows)]
            return remote(m, n, part, part, right)
        if n == 3:
            part = buf.at[right, pl.ds(n_rows, n_rows)]
            return remote(m, n, part, part, left)
        if n == 4:
            return remote(m, n, own, buf.at[me], other)
        dev = (left, right, far)[n - 5]
        return remote(m, n, buf.at[dev], buf.at[dev], other)

    def send_own(m):
        for n in (0, 1, 4):
            copy(m, n).start()

    def pass_on(m):
        for n in (0, 1):
            copy(m, n).wait_recv()
            copy(m, 2 + n).start()
            copy(m, 5 + n).start()

    def pass_far(m):
        for n in (2, 3):
            copy(m, n).wait_recv()
        copy(m, 7).start()

    def seq_id(i, t):
        return ids_ref[t * per + core * steps + i]

    def tile(i):
        return pl.ds(pl.multiple_of(i * M, M), M)

    x_base = 4

    def a_copies(dev, src, n):
        out = []
        for pr in range(3):
            for a in range(n_ad):
                k = pr * n_ad + a
                o = pl.multiple_of(dev * rl, rl)
                dst = attn.at[a, pl.ds(pr * rank + o, rl)] if pr < 2 else attn.at[n_ad + a, pl.ds(o, rl)]
                out.append(pltpu.make_async_copy(src.at[pl.ds(k * rl, rl)], dst, asem.at[n, k]))
        return out

    def w_copies(r):
        out = []
        for n, c in enumerate((core, 1 - core)):
            src = w_own if r == 0 and n == 0 else gw.at[order[r] * CORES + c]
            out.append(pltpu.make_async_copy(src, w.at[r, pl.ds(pl.multiple_of(c * dw, dw), dw)], wsem.at[r, n, 0]))
        return out

    def b_copies(r):
        out = []
        for n, c in enumerate((core, 1 - core)):
            src = b_own if r == 0 and n == 0 else gb.at[order[r] * CORES + c]
            for a in range(n_ad):
                out.append(pltpu.make_async_copy(src.at[pl.ds(a * dw, dw)],
                                                 bw.at[r, a, pl.ds(pl.multiple_of(c * dw, dw), dw)], wsem.at[r, n, 1 + a]))
        return out

    def x_copies(i, slot):
        return [pltpu.make_async_copy(x_ref.at[t, core * steps + i],
                                      attn.at[x_base + slot, pl.ds(t * S, S)], xsem.at[slot, t])
                for t in range(chips)]

    send_own(0)
    for c in x_copies(0, 0):
        c.start()
    rb = 16

    @pl.loop(0, steps)
    def _(i):
        slot = i % 2
        for c in x_copies(i, slot):
            c.wait()

        @pl.when(i + 1 < steps)
        def _():
            for c in x_copies(i + 1, 1 - slot):
                c.start()

        @pl.loop(0, M // rb)
        def _(r):
            v = attn[x_base + slot, pl.ds(pl.multiple_of(r * rb, rb), rb), :].astype(F32)
            inv = lax.rsqrt(jnp.mean(v * v, axis=-1, keepdims=True) + EPSILON)
            h[pl.ds(pl.multiple_of(i * M + r * rb, rb), rb), :] = (v * inv * gain_ref[...]).astype(BF16)

    pass_on(0)
    send_own(1)
    send_own(2)
    devs = [order[r] * CORES + c for r in range(chips) for c in (core, 1 - core)]
    pass_far(0)
    for n in range(4):
        copy(0, 4 + n).wait_recv()
    stacks = [c for n, dev in enumerate(devs) for c in a_copies(dev, a_own if n == 0 else ga.at[dev], n)]
    for c in stacks:
        c.start()
    for c in stacks:
        c.wait()

    @pl.loop(0, steps)
    def _(i):
        for t in range(chips):
            rows = pl.ds(pl.multiple_of(i * M + t * S, S), S)
            idx = seq_id(i, t)
            low[rows, :2 * rank] = dot_nt(h[rows, :], attn[idx]).astype(BF16)
            low[rows, 2 * rank:] = dot_nt(h[rows, :], attn[n_ad + idx, :rank]).astype(BF16)

    def produce(it, slot):
        r, i = it // steps, it % steps
        z = dot_nt(w[r], h[tile(i), :])
        for t in range(chips):
            rows = pl.ds(pl.multiple_of(i * M + t * S, S), S)
            b = bw[r, seq_id(i, t)]
            lo = low[rows, :]
            cols = slice(t * S, (t + 1) * S)

            def project(o, n, c0):
                zz = jnp.concatenate([z[c * dw + o:c * dw + o + n, cols] for c in range(CORES)], axis=0)
                bb = jnp.concatenate([b[c * dw + o:c * dw + o + n] for c in range(CORES)], axis=0)
                return zz + scale * dot_nt(bb, lo[:, c0:c0 + rank])

            zq, zk, zv = project(0, qw, 0), project(qw, hd, rank), project(qw + hd, hd, 2 * rank)
            cos, sin = cos_ref[...], sin_ref[...]

            def rotate(v):
                f, s = v[:half], v[half:]
                return jnp.concatenate([f * cos - s * sin, s * cos + f * sin], axis=0)

            for hh in range(CORES * nq):
                o = hh * hd
                q_scr[slot, o:o + hd, cols] = (rotate(zq[o:o + hd]) * hd ** -0.5).astype(BF16)
            kt = jnp.concatenate([rotate(zk[c * hd:(c + 1) * hd]) for c in range(CORES)], axis=0)
            kk = kt.T.astype(BF16)
            for c in range(CORES):
                k_scr[slot, c, t * S:(t + 1) * S, :] = kk[:, c * hd:(c + 1) * hd]
            v_scr[slot, :, cols] = zv.astype(BF16)

    def consume(it, slot):
        r, i = it // steps, it % steps
        p = (chip + r) % chips
        key = lax.broadcasted_iota(jnp.int32, (S, S), 0)
        qry = lax.broadcasted_iota(jnp.int32, (S, S), 1)
        causal = key <= qry
        for c in range(CORES):
            for t in range(chips):
                cols = slice(t * S, (t + 1) * S)
                q = jnp.concatenate([q_scr[slot, c * qw + hh * hd:c * qw + (hh + 1) * hd, cols] for hh in range(nq)], axis=1)
                sc = dot_nn(k_scr[slot, c, cols, :], q)
                ps = []
                for hh in range(nq):
                    sh = jnp.where(causal, sc[:, hh * S:(hh + 1) * S], -1e30)
                    e = jnp.exp(sh - jnp.max(sh, axis=0, keepdims=True))
                    ps.append((e * (1.0 / jnp.sum(e, axis=0, keepdims=True))).astype(BF16))
                o = dot_nn(v_scr[slot, c * hd:(c + 1) * hd, cols], jnp.concatenate(ps, axis=1))
                o = jnp.concatenate([o[:, hh * S:(hh + 1) * S] for hh in range(nq)], axis=0)
                attn[i, pl.ds(t * S, S),
                     pl.ds(pl.multiple_of((p * CORES + c) * qw, qw), qw)] = o.T.astype(BF16)

    def out_copy(i):
        return pltpu.make_async_copy(attn.at[i], out_ref.at[i], osem.at[i])

    for m in (1, 2):
        copy(m, 4).wait_recv()
    for c in w_copies(0) + b_copies(0):
        c.start()
    for c in w_copies(0) + b_copies(0):
        c.wait()
    produce(0, 0)

    @pl.loop(0, chips * steps)
    def _(it):
        nxt = jnp.minimum(it + 1, chips * steps - 1)

        @pl.when(it == 2)
        def _():
            pass_on(1)
            pass_on(2)

        @pl.when(it == steps)
        def _():
            pass_far(1)
            pass_far(2)
        for r in range(1, chips):
            @pl.when(it == r * steps - 2)
            def _():
                for m in (1, 2):
                    copy(m, (4, 6, 7, 5)[r]).wait_recv()
                for c in w_copies(r):
                    c.start()

            @pl.when(it == r * steps - 1)
            def _():
                for c in b_copies(r):
                    c.start()
                for c in w_copies(r) + b_copies(r):
                    c.wait()
        consume(it, it % 2)

        @pl.when(it >= (chips - 1) * steps)
        def _():
            out_copy(it % steps).start()
        produce(nxt, (it + 1) % 2)

    for i in range(steps):
        out_copy(i).wait()
    for m in range(3):
        for n in range(8):
            copy(m, n).wait_send()


def oproj_body(dims, meta, attn_ref, x_ref, gwo_ref, gb_ref, out_ref, wo, ao, bo, low, sems):
    n_dev, seqs, S, qw, rank, D, chips = dims
    n_ad = 2
    scale = ALPHA / rank
    step = pl.program_id(0)
    core = meta[seqs]
    per = seqs // chips
    steps = per // CORES
    plan = [(gwo_ref, wo)]
    for d in range(n_dev):
        for a in range(n_ad):
            plan.append((gb_ref.at[d, pl.ds(a * qw, qw)], ao.at[a, pl.ds(d * qw, qw)]))
            plan.append((gb_ref.at[d, pl.ds(n_ad * qw + a * rank, rank)], bo.at[a, :, pl.ds(d * qw, qw)]))

    @pl.when(step == 0)
    def _():
        for s, d in plan:
            pltpu.make_async_copy(s, d, sems.at[0]).start()
        for s, d in plan:
            pltpu.make_async_copy(s, d, sems.at[0]).wait()

    ids = [meta[t * per + core * steps + step] for t in range(chips)]
    for t in range(chips):
        low[pl.ds(t * S, S), :] = dot_nn(attn_ref[0, pl.ds(t * S, S), :], ao[ids[t]]).astype(BF16)
    nt = 256

    @pl.loop(0, D // nt)
    def _(j):
        cols = pl.ds(pl.multiple_of(j * nt, nt), nt)
        zo = dot_nn(attn_ref[0], wo[:, cols])
        for t in range(chips):
            z = zo[t * S:(t + 1) * S] + scale * dot_nn(low[pl.ds(t * S, S), :], bo[ids[t], :, cols])
            out_ref[t, 0, :, cols] = (x_ref[t, 0, :, cols].astype(F32) + z).astype(BF16)


def mlp_body(dims, ids_ref, x_ref, gain_ref, agu_ref, wg0, wg1, wu0, wu1, wd0, wd1, bg0, bg1, bu0, bu1, ad0, ad1, bd_ref,
             y_ref, wg, wu, wd, bg, bu, agu, ad, bd, xt, h_scr, low_scr, hid_scr, part, in_a, in_b, xo, ybuf,
             wsem, xsem, osem, sa, ra, sb, rb_, sy, ry, sf, rf, sp, rp):
    seqs, S, rank, D, chips = dims
    scale = ALPHA / rank
    fw = wg0.shape[1]
    per = seqs // chips
    steps = per // CORES
    M = chips * S
    hs = S // 2
    me = lax.axis_index('tensor')
    core, chip = me % CORES, me // CORES
    right_chip, left_chip = (chip + 1) % chips, (chip + chips - 1) % chips
    far_chip = (chip + 2) % chips
    right, left, other = right_chip * CORES + core, left_chip * CORES + core, chip * CORES + (1 - core)

    barrier = pltpu.get_barrier_semaphore()
    for dev in (right, left, other):
        pl.semaphore_signal(barrier, inc=1, device_id={'tensor': dev}, device_id_type=pl.DeviceIdType.MESH)
    pl.semaphore_wait(barrier, 3)

    def remote(src, dst, ssem, rsem, dev):
        return pltpu.make_async_remote_copy(src_ref=src, dst_ref=dst, send_sem=ssem, recv_sem=rsem,
                                            device_id={'tensor': dev}, device_id_type=pl.DeviceIdType.MESH)

    def copies_a(j):
        s, r = j % 3, j % 4
        return [remote(part.at[s, far_chip, pl.ds(0, hs)], in_a.at[0, r], sa.at[0, j], ra.at[0, j], right),
                remote(part.at[s, far_chip, pl.ds(hs, hs)], in_a.at[1, r], sa.at[1, j], ra.at[1, j], left)]

    def copies_b(j):
        s, r = j % 3, j % 3
        return [remote(part.at[s, right_chip], in_b.at[0, r], sb.at[0, j], rb_.at[0, j], right),
                remote(part.at[s, left_chip], in_b.at[1, r], sb.at[1, j], rb_.at[1, j], left)]

    def copies_y(j):
        dst = y_ref.at[me, j]
        src = ybuf.at[j % 2]
        return [remote(src, dst, sy.at[0, j], ry.at[0, j], right), remote(src, dst, sy.at[1, j], ry.at[1, j], left)]

    def copies_f(j):
        from_left = y_ref.at[left, j, pl.ds(0, hs)]
        from_right = y_ref.at[right, j, pl.ds(hs, hs)]
        return [remote(from_left, from_left, sf.at[0, j], rf.at[0, j], right),
                remote(from_right, from_right, sf.at[1, j], rf.at[1, j], left)]

    far = far_chip * CORES + core

    def copies_p(j):
        out = [remote(ybuf.at[j % 2], y_ref.at[me, j], sp.at[0, j], rp.at[0, j], other)]
        for n, dev in enumerate((left, right, far)):
            out.append(remote(y_ref.at[dev, j], y_ref.at[dev, j], sp.at[n + 1, j], rp.at[n + 1, j], other))
        return out

    def store_y(j):
        return pltpu.make_async_copy(ybuf.at[j % 2], y_ref.at[me, j], osem.at[j % 2])

    plans = [[(agu_ref, agu)], [], [(bd_ref, bd)]]
    for i, (g, u, b1, b2) in enumerate(((wg0, wu0, bg0, bu0), (wg1, wu1, bg1, bu1))):
        c = pl.ds(i * fw, fw)
        plans[1] += [(g, wg.at[:, c]), (u, wu.at[:, c]), (b1, bg.at[:, :, c]), (b2, bu.at[:, :, c])]
    for i, (d, a) in enumerate(((wd0, ad0), (wd1, ad1))):
        c = pl.ds(i * fw, fw)
        plans[2] += [(a, ad.at[:, c]), (d, wd.at[c])]
    n_plan = [0]
    flat = []
    for plan in plans:
        group = []
        for src, dst in plan:
            group.append(pltpu.make_async_copy(src, dst, wsem.at[n_plan[0]]))
            n_plan[0] += 1
        flat.append(group)

    def x_copy(i, slot):
        return pltpu.make_async_copy(x_ref.at[:, i], xt.at[slot], xsem.at[slot])

    def xo_copy(i):
        return pltpu.make_async_copy(x_ref.at[chip, i], xo.at[i % 2], xsem.at[2 + i % 2])

    x_copy(0, 0).start()
    for group in flat:
        for c in group:
            c.start()

    def arrive(i, step):
        @pl.when(step == 0)
        def _():
            for c in flat[i]:
                c.wait()

    nt = 256
    rb = 16

    def compute(k):
        slot = k % 2
        x_copy(k, slot).wait()

        @pl.when(k + 1 < steps)
        def _():
            x_copy(k + 1, 1 - slot).start()

        ids = [ids_ref[t * per + core * steps + k] for t in range(chips)]

        @pl.loop(0, M // rb)
        def _(i):
            t, r = i // (S // rb), i % (S // rb)
            v = xt[slot, t, pl.ds(pl.multiple_of(r * rb, rb), rb), :].astype(F32)
            inv = lax.rsqrt(jnp.mean(v * v, axis=-1, keepdims=True) + EPSILON)
            h_scr[pl.ds(pl.multiple_of(i * rb, rb), rb), :] = (v * inv * gain_ref[...]).astype(BF16)

        arrive(0, k)
        for t in range(chips):
            low_scr[pl.ds(t * S, S), :] = dot_nn(h_scr[pl.ds(t * S, S), :], agu[ids[t]]).astype(BF16)
        arrive(1, k)

        @pl.loop(0, wg.shape[1] // nt)
        def _(j):
            cols = pl.ds(pl.multiple_of(j * nt, nt), nt)
            zg = dot_nn(h_scr[...], wg[:, cols])
            zu = dot_nn(h_scr[...], wu[:, cols])
            for t in range(chips):
                rows = pl.ds(t * S, S)
                g = zg[t * S:(t + 1) * S] + scale * dot_nn(low_scr[rows, :rank], bg[ids[t], :, cols])
                u = zu[t * S:(t + 1) * S] + scale * dot_nn(low_scr[rows, rank:], bu[ids[t], :, cols])
                hid_scr[rows, cols] = (jax.nn.silu(g) * u).astype(BF16)

        arrive(2, k)

        @pl.when(k >= 3)
        def _():
            for c in copies_a(k - 3) + copies_b(k - 3):
                c.wait_send()
        s = k % 3
        for t in range(chips):
            part[s, t, :, D:] = dot_nn(hid_scr[pl.ds(t * S, S), :], ad[ids[t]]).astype(BF16)

        @pl.loop(0, D // nt)
        def _(j):
            cols = pl.ds(pl.multiple_of(j * nt, nt), nt)
            z = dot_nn(hid_scr[...], wd[:, cols])
            for t in range(chips):
                part[s, t, :, cols] = z[t * S:(t + 1) * S].astype(BF16)

        for c in copies_a(k):
            c.start()

    def relay(j):
        s, r = j % 3, j % 4
        for n, (dest, lo) in enumerate(((right_chip, 0), (left_chip, hs))):
            copies_a(j)[n].wait_recv()

            @pl.loop(0, hs // rb)
            def _(i):
                rows = pl.ds(pl.multiple_of(lo + i * rb, rb), rb)
                got = in_a[n, r, pl.ds(pl.multiple_of(i * rb, rb), rb), :]
                part[s, dest, rows, :] = (part[s, dest, rows, :].astype(F32) + got.astype(F32)).astype(BF16)
            copies_b(j)[n].start()
        xo_copy(j).start()

    def settle(j):
        s = j % 3
        for c in copies_b(j):
            c.wait_recv()
        xo_copy(j).wait()

        @pl.when(j >= 2)
        def _():
            store_y(j - 2).wait()
            for c in copies_y(j - 2) + copies_p(j - 2)[:1]:
                c.wait_send()
        idx = ids_ref[chip * per + core * steps + j]

        def total(cols):
            return (part[s, chip, :, cols].astype(F32) + in_b[0, s, :, cols].astype(F32)) + in_b[1, s, :, cols].astype(F32)

        low = total(pl.ds(D, rank)).astype(BF16)

        @pl.loop(0, D // nt)
        def _(i):
            cols = pl.ds(pl.multiple_of(i * nt, nt), nt)
            z = total(cols) + scale * dot_nn(low, bd[idx, :, cols])
            ybuf[j % 2, :, cols] = (xo[j % 2, :, cols].astype(F32) + z).astype(BF16)
        store_y(j).start()
        for c in copies_y(j) + copies_p(j)[:1]:
            c.start()

    def forward(j):
        for n in range(2):
            copies_y(j)[n].wait_recv()
            copies_f(j)[n].start()
            copies_p(j)[1 + n].start()

    def last_hop(j):
        for c in copies_f(j):
            c.wait_recv()
        copies_p(j)[3].start()

    @pl.loop(0, steps + 4)
    def _(k):
        @pl.when(k < steps)
        def _():
            compute(k)
        for lag, stage in ((1, relay), (2, settle), (3, forward), (4, last_hop)):
            @pl.when((k >= lag) & (k < steps + lag))
            def _():
                stage(k - lag)

    for j in range(max(0, steps - 3), steps):
        for c in copies_a(j) + copies_b(j):
            c.wait_send()
    for j in range(max(0, steps - 2), steps):
        store_y(j).wait()
        for c in copies_y(j) + copies_p(j)[:1]:
            c.wait_send()

    @pl.loop(0, steps)
    def _(j):
        for c in copies_f(j) + copies_p(j)[1:]:
            c.wait_send()
        for c in copies_p(j):
            c.wait_recv()


def solution(mesh):
    n_dev = mesh.shape['tensor']
    chips = n_dev // CORES
    head_split = P(None, 'tensor', None)
    last_split = P(None, None, 'tensor')
    b_head_split = P(None, None, 'tensor', None)
    in_specs = (P('data', None, None), P('data'), P(None), P(None),
                head_split, head_split, head_split, P('tensor', None, None),
                P(None, 'tensor'), P(None, 'tensor'), P('tensor', None),
                last_split, b_head_split, last_split, b_head_split, last_split, b_head_split,
                P(None, 'tensor', None, None), last_split,
                last_split, last_split, last_split, last_split,
                P(None, 'tensor', None), last_split)
    swap = [(i, i ^ 1) for i in range(n_dev)]
    ANY = pl.BlockSpec(memory_space=pl.ANY)

    def local_layer(x_in, adapter_ids, gain_attn, gain_mlp, w_q, w_k, w_v, w_o, w_gate, w_up, w_down, a_q, b_q, a_k, b_k, a_v, b_v, a_o, b_o, a_gate, b_gate, a_up, b_up, a_down, b_down):
        seqs, S, D = x_in.shape
        nq, hd = w_q.shape[1], w_q.shape[2]
        n_ad, rank = b_q.shape[0], b_q.shape[1]
        rl = a_q.shape[2]
        half = hd // 2
        qw = nq * hd
        per = seqs // chips
        steps = per // CORES

        def rows_t(w):
            return jnp.transpose(w, (1, 2, 0)).reshape(-1, w.shape[0])

        gather = functools.partial(lax.all_gather, axis_name='tensor', axis=0)
        swapped = functools.partial(lax.ppermute, axis_name='tensor', perm=swap)

        def rows_a(stacks):
            return jnp.concatenate([jnp.transpose(a, (0, 2, 1)).reshape(n_ad * rl, D) for a in stacks], axis=0)

        def b_rows(b):
            return jnp.transpose(b, (1, 2, 0)).reshape(-1, rank)

        a_own = rows_a((a_q, a_k, a_v))
        w_own = jnp.concatenate([rows_t(w_q), rows_t(w_k), rows_t(w_v)], axis=0)
        b_own = jnp.concatenate([b_rows(b[a]) for a in range(n_ad) for b in (b_q, b_k, b_v)], axis=0)
        g_wo = gather(w_o.reshape(qw, D))
        g_b = gather(jnp.concatenate([a_o.reshape(n_ad * qw, rank), b_o.reshape(n_ad * rank, qw),
                                      b_down.reshape(n_ad * rank, qw)], axis=0))
        bd_full = g_b[:, n_ad * (qw + rank):].reshape(n_dev, n_ad, rank, qw).transpose(1, 2, 0, 3).reshape(n_ad, rank, D)
        g_gu = gather(rows_a((a_gate, a_up))).reshape(n_dev, 2, n_ad, rl, D)
        a_gu = g_gu.transpose(2, 4, 1, 0, 3).reshape(n_ad, D, 2 * rank)
        mlp_own = (w_gate, w_up, w_down, b_gate, b_up, a_down)
        mlp_other = tuple(swapped(w) for w in mlp_own)

        inv_freq = ROPE_BASE ** (-2.0 * jnp.arange(half, dtype=F32) / hd)
        ang = jnp.arange(S, dtype=F32)[:, None] * inv_freq[None, :]
        cos, sin = jnp.cos(ang), jnp.sin(ang)
        cos_t, sin_t = cos.T, sin.T

        x4 = x_in.reshape(chips, per, S, D)
        M = chips * S
        Fc = CORES * w_gate.shape[1]
        dma = pltpu.SemaphoreType.DMA
        dw = qw + 2 * hd
        attn_all = pl.pallas_call(
            functools.partial(attn_body, (n_dev, seqs, S, hd, nq, rank, D, chips)),
            in_specs=[pl.BlockSpec(memory_space=pltpu.SMEM), ANY] + [pl.BlockSpec(memory_space=pltpu.VMEM)] * 3 + [ANY] * 3,
            out_specs=[ANY] * 4,
            scratch_shapes=[
                pltpu.VMEM((steps * M, D), BF16), pltpu.VMEM((steps * M, 3 * rank), BF16), pltpu.VMEM((steps, M, n_dev * qw), BF16),
                pltpu.VMEM((chips, CORES * dw, D), BF16), pltpu.VMEM((chips, n_ad, CORES * dw, rank), BF16),
                pltpu.VMEM((2, CORES * qw, M), BF16), pltpu.VMEM((2, CORES, M, hd), BF16), pltpu.VMEM((2, CORES * hd, M), BF16),
                dma((n_dev, 3 * n_ad)), dma((chips, CORES, 1 + n_ad)), dma((2, chips)), dma((steps,)), dma((3, 8)), dma((3, 8))],
            out_shape=[jax.ShapeDtypeStruct((steps, M, n_dev * qw), BF16), jax.ShapeDtypeStruct((n_dev,) + a_own.shape, BF16),
                       jax.ShapeDtypeStruct((n_dev,) + w_own.shape, BF16), jax.ShapeDtypeStruct((n_dev,) + b_own.shape, BF16)],
            compiler_params=pltpu.CompilerParams(vmem_limit_bytes=VMEM_LIMIT, collective_id=1, has_side_effects=True),
            name="attn_ring",
            cost_estimate=pl.CostEstimate(flops=3 * steps * M * D * (n_dev * qw + 2 * n_dev * hd + 3 * rank),
                                          bytes_accessed=6 * steps * M * D + 33 * 2**20, transcendentals=0),
        )(adapter_ids, x4, gain_attn.reshape(1, D), cos_t, sin_t, a_own, w_own, b_own)[0]
        core = lax.axis_index('tensor') % CORES
        meta = jnp.concatenate([adapter_ids.astype(jnp.int32), core.reshape(1).astype(jnp.int32)])
        x1_all = pl.pallas_call(
            functools.partial(oproj_body, (n_dev, seqs, S, qw, rank, D, chips)),
            grid_spec=pltpu.PrefetchScalarGridSpec(
                num_scalar_prefetch=1, grid=(steps,),
                in_specs=[pl.BlockSpec((1, M, n_dev * qw), lambda i, m: (i, 0, 0)),
                          pl.BlockSpec((chips, 1, S, D), lambda i, m: (0, m[seqs] * steps + i, 0, 0)), ANY, ANY],
                out_specs=pl.BlockSpec((chips, 1, S, D), lambda i, m: (0, i, 0, 0)),
                scratch_shapes=[pltpu.VMEM((n_dev * qw, D), BF16), pltpu.VMEM((n_ad, n_dev * qw, rank), BF16),
                                pltpu.VMEM((n_ad, rank, D), BF16), pltpu.VMEM((M, rank), BF16), dma((1,))]),
            out_shape=jax.ShapeDtypeStruct((chips, steps, S, D), BF16),
            compiler_params=pltpu.CompilerParams(vmem_limit_bytes=VMEM_LIMIT, dimension_semantics=("arbitrary",)), name="oproj",
            cost_estimate=pl.CostEstimate(flops=2 * steps * M * D * (D + 2 * rank),
                                          bytes_accessed=6 * steps * M * D + 12 * 2**20, transcendentals=0),
        )(meta, attn_all, x4, g_wo.reshape(n_dev * qw, D), g_b)
        pairs = [w for own, other in zip(mlp_own, mlp_other) for w in (own, other)]
        y = pl.pallas_call(
            functools.partial(mlp_body, (seqs, S, rank, D, chips)),
            in_specs=[pl.BlockSpec(memory_space=pltpu.SMEM), ANY, pl.BlockSpec(memory_space=pltpu.VMEM)] + [ANY] * 14,
            out_specs=ANY,
            scratch_shapes=[
                pltpu.VMEM((D, Fc), BF16), pltpu.VMEM((D, Fc), BF16), pltpu.VMEM((Fc, D), BF16),
                pltpu.VMEM((n_ad, rank, Fc), BF16), pltpu.VMEM((n_ad, rank, Fc), BF16),
                pltpu.VMEM((n_ad, D, 2 * rank), BF16), pltpu.VMEM((n_ad, Fc, rank), BF16), pltpu.VMEM((n_ad, rank, D), BF16),
                pltpu.VMEM((2, chips, S, D), BF16), pltpu.VMEM((M, D), BF16), pltpu.VMEM((M, 2 * rank), BF16), pltpu.VMEM((M, Fc), BF16),
                pltpu.VMEM((3, chips, S, D + rank), BF16), pltpu.VMEM((2, 4, S // 2, D + rank), BF16),
                pltpu.VMEM((2, 3, S, D + rank), BF16), pltpu.VMEM((2, S, D), BF16), pltpu.VMEM((2, S, D), BF16),
                dma((14,)), dma((4,)), dma((2,)), dma((2, steps)), dma((2, steps)), dma((2, steps)), dma((2, steps)),
                dma((2, steps)), dma((2, steps)), dma((2, steps)), dma((2, steps)), dma((4, steps)), dma((4, steps))],
            out_shape=jax.ShapeDtypeStruct((n_dev, steps, S, D), BF16),
            compiler_params=pltpu.CompilerParams(vmem_limit_bytes=VMEM_LIMIT, collective_id=0, has_side_effects=True),
            name="mlp_ring",
            cost_estimate=pl.CostEstimate(flops=2 * steps * M * D * (3 * Fc + 4 * rank),
                                          bytes_accessed=8 * steps * M * D + 34 * 2**20, transcendentals=steps * M * Fc),
        )(adapter_ids, x1_all, gain_mlp.reshape(1, D), a_gu, *pairs, bd_full)
        return y.reshape(seqs, S, D)

    return jax.shard_map(local_layer, mesh=mesh, in_specs=in_specs, out_specs=P('data', None, None), check_vma=False)
```

```python
import functools

import jax
import jax.numpy as jnp
from jax import lax
from jax.experimental import pallas as pl
from jax.experimental.pallas import tpu as pltpu
from jax.sharding import PartitionSpec as P

ALPHA = 16.0
ROPE_BASE = 10000.0
EPSILON = 1e-5
CORES = 2
VMEM_LIMIT = 62 * 1024 * 1024
F32, BF16 = jnp.float32, jnp.bfloat16


def dot_nn(a, b):
    return lax.dot_general(a, b, (((1,), (0,)), ((), ())), preferred_element_type=F32)


def dot_nt(a, b):
    return lax.dot_general(a, b, (((1,), (1,)), ((), ())), preferred_element_type=F32)


def attn_body(dims, ids_ref, x_ref, gain_ref, cos_ref, sin_ref, a_own, w_own, b_own, out_ref, ga, gw, gb,
              h, low, attn, w, bw, q_scr, k_scr, v_scr, asem, wsem, xsem, osem, ss, rs):
    n_dev, seqs, S, hd, nq, rank, D, chips = dims
    half = hd // 2
    qw = nq * hd
    n_ad = 2
    scale = ALPHA / rank
    me = lax.axis_index('tensor')
    core, chip = me % CORES, me // CORES
    per = seqs // chips
    steps = per // CORES
    M = chips * S
    dw = qw + 2 * hd
    rl = rank // n_dev
    right_chip, left_chip, far_chip = (chip + 1) % chips, (chip + chips - 1) % chips, (chip + 2) % chips
    order = [(chip + r) % chips for r in range(chips)]
    right, left, far = [c * CORES + core for c in (right_chip, left_chip, far_chip)]
    other = chip * CORES + (1 - core)

    barrier = pltpu.get_barrier_semaphore()
    for dev in (right, left, other):
        pl.semaphore_signal(barrier, inc=1, device_id={'tensor': dev}, device_id_type=pl.DeviceIdType.MESH)
    pl.semaphore_wait(barrier, 3)

    groups = ((a_own, ga), (w_own, gw), (b_own, gb))

    def remote(m, n, src, dst, dev):
        return pltpu.make_async_remote_copy(src_ref=src, dst_ref=dst, send_sem=ss.at[m, n], recv_sem=rs.at[m, n],
                                            device_id={'tensor': dev}, device_id_type=pl.DeviceIdType.MESH)

    def copy(m, n):
        own, buf = groups[m]
        n_rows = own.shape[0] // 2
        if n == 0:
            return remote(m, n, own, buf.at[me], right)
        if n == 1:
            return remote(m, n, own, buf.at[me], left)
        if n == 2:
            part = buf.at[left, pl.ds(0, n_rows)]
            return remote(m, n, part, part, right)
        if n == 3:
            part = buf.at[right, pl.ds(n_rows, n_rows)]
            return remote(m, n, part, part, left)
        if n == 4:
            return remote(m, n, own, buf.at[me], other)
        dev = (left, right, far)[n - 5]
        return remote(m, n, buf.at[dev], buf.at[dev], other)

    def send_own(m):
        for n in (0, 1, 4):
            copy(m, n).start()

    def pass_on(m):
        for n in (0, 1):
            copy(m, n).wait_recv()
            copy(m, 2 + n).start()
            copy(m, 5 + n).start()

    def pass_far(m):
        for n in (2, 3):
            copy(m, n).wait_recv()
        copy(m, 7).start()

    def seq_id(i, t):
        return ids_ref[t * per + core * steps + i]

    x_base = 4

    def a_copies(dev, src, n):
        out = []
        for pr in range(3):
            for a in range(n_ad):
                k = pr * n_ad + a
                o = pl.multiple_of(dev * rl, rl)
                dst = attn.at[a, pl.ds(pr * rank + o, rl)] if pr < 2 else attn.at[n_ad + a, pl.ds(o, rl)]
                out.append(pltpu.make_async_copy(src.at[pl.ds(k * rl, rl)], dst, asem.at[n, k]))
        return out

    def w_copies(r):
        out = []
        for n, c in enumerate((core, 1 - core)):
            src = w_own if r == 0 and n == 0 else gw.at[order[r] * CORES + c]
            out.append(pltpu.make_async_copy(src, w.at[r, pl.ds(pl.multiple_of(c * dw, dw), dw)], wsem.at[r, n, 0]))
        return out

    def b_copies(r):
        out = []
        for n, c in enumerate((core, 1 - core)):
            src = b_own if r == 0 and n == 0 else gb.at[order[r] * CORES + c]
            for a in range(n_ad):
                out.append(pltpu.make_async_copy(src.at[pl.ds(a * dw, dw)],
                                                 bw.at[r, a, pl.ds(pl.multiple_of(c * dw, dw), dw)], wsem.at[r, n, 1 + a]))
        return out

    def x_copies(i, slot):
        return [pltpu.make_async_copy(x_ref.at[t, core * steps + i],
                                      attn.at[x_base + slot, pl.ds(t * S, S)], xsem.at[slot, t])
                for t in range(chips)]

    send_own(0)
    for c in x_copies(0, 0):
        c.start()
    rb = 16

    @pl.loop(0, steps)
    def _(i):
        slot = i % 2
        for c in x_copies(i, slot):
            c.wait()

        @pl.when(i + 1 < steps)
        def _():
            for c in x_copies(i + 1, 1 - slot):
                c.start()

        @pl.loop(0, M // rb)
        def _(r):
            v = attn[x_base + slot, pl.ds(pl.multiple_of(r * rb, rb), rb), :].astype(F32)
            inv = lax.rsqrt(jnp.mean(v * v, axis=-1, keepdims=True) + EPSILON)
            attn[x_base + 2, pl.ds(pl.multiple_of(r * rb, rb), rb), :] = (v * inv * gain_ref[...]).astype(BF16)

        @pl.loop(0, D // S)
        def _(c):
            block = pl.ds(pl.multiple_of(c * S, S), S)
            h[i, block, :] = attn[x_base + 2, :, block].T

    pass_on(0)
    send_own(1)
    send_own(2)
    devs = [order[r] * CORES + c for r in range(chips) for c in (core, 1 - core)]
    pass_far(0)
    for n in range(4):
        copy(0, 4 + n).wait_recv()
    stacks = [c for n, dev in enumerate(devs) for c in a_copies(dev, a_own if n == 0 else ga.at[dev], n)]
    for c in stacks:
        c.start()
    for c in stacks:
        c.wait()

    @pl.loop(0, steps)
    def _(i):
        for t in range(chips):
            idx = seq_id(i, t)
            cols = slice(t * S, (t + 1) * S)
            low[i, :2 * rank, cols] = dot_nn(attn[idx], h[i, :, cols]).astype(BF16)
            low[i, 2 * rank:, cols] = dot_nn(attn[n_ad + idx, :rank], h[i, :, cols]).astype(BF16)

    def produce(it, slot):
        r, i = it // steps, it % steps
        z = dot_nn(w[r], h[i])
        for t in range(chips):
            b = bw[r, seq_id(i, t)]
            cols = slice(t * S, (t + 1) * S)

            def project(o, n, c0):
                zz = jnp.concatenate([z[c * dw + o:c * dw + o + n, cols] for c in range(CORES)], axis=0)
                bb = jnp.concatenate([b[c * dw + o:c * dw + o + n] for c in range(CORES)], axis=0)
                return zz + scale * dot_nn(bb, low[i, c0:c0 + rank, cols])

            zq, zk, zv = project(0, qw, 0), project(qw, hd, rank), project(qw + hd, hd, 2 * rank)
            cos, sin = cos_ref[...], sin_ref[...]

            def rotate(v):
                f, s = v[:half], v[half:]
                return jnp.concatenate([f * cos - s * sin, s * cos + f * sin], axis=0)

            for hh in range(CORES * nq):
                o = hh * hd
                q_scr[slot, o:o + hd, cols] = (rotate(zq[o:o + hd]) * hd ** -0.5).astype(BF16)
            kt = jnp.concatenate([rotate(zk[c * hd:(c + 1) * hd]) for c in range(CORES)], axis=0)
            kk = kt.T.astype(BF16)
            for c in range(CORES):
                k_scr[slot, c, t * S:(t + 1) * S, :] = kk[:, c * hd:(c + 1) * hd]
            v_scr[slot, :, cols] = zv.astype(BF16)

    def consume(it, slot):
        r, i = it // steps, it % steps
        p = (chip + r) % chips
        key = lax.broadcasted_iota(jnp.int32, (S, S), 0)
        qry = lax.broadcasted_iota(jnp.int32, (S, S), 1)
        causal = key <= qry
        for c in range(CORES):
            for t in range(chips):
                cols = slice(t * S, (t + 1) * S)
                q = jnp.concatenate([q_scr[slot, c * qw + hh * hd:c * qw + (hh + 1) * hd, cols] for hh in range(nq)], axis=1)
                sc = dot_nn(k_scr[slot, c, cols, :], q)
                ps = []
                for hh in range(nq):
                    sh = jnp.where(causal, sc[:, hh * S:(hh + 1) * S], -1e30)
                    e = jnp.exp(sh - jnp.max(sh, axis=0, keepdims=True))
                    ps.append((e * (1.0 / jnp.sum(e, axis=0, keepdims=True))).astype(BF16))
                o = dot_nn(v_scr[slot, c * hd:(c + 1) * hd, cols], jnp.concatenate(ps, axis=1))
                o = jnp.concatenate([o[:, hh * S:(hh + 1) * S] for hh in range(nq)], axis=0)
                attn[i, pl.ds(t * S, S),
                     pl.ds(pl.multiple_of((p * CORES + c) * qw, qw), qw)] = o.T.astype(BF16)

    def out_copy(i):
        return pltpu.make_async_copy(attn.at[i], out_ref.at[i], osem.at[i])

    for m in (1, 2):
        copy(m, 4).wait_recv()
    for c in w_copies(0) + b_copies(0):
        c.start()
    for c in w_copies(0) + b_copies(0):
        c.wait()
    produce(0, 0)

    @pl.loop(0, chips * steps)
    def _(it):
        nxt = jnp.minimum(it + 1, chips * steps - 1)

        @pl.when(it == 2)
        def _():
            pass_on(1)
            pass_on(2)

        @pl.when(it == steps)
        def _():
            pass_far(1)
            pass_far(2)
        for r in range(1, chips):
            @pl.when(it == r * steps - 2)
            def _():
                for m in (1, 2):
                    copy(m, (4, 6, 7, 5)[r]).wait_recv()
                for c in w_copies(r):
                    c.start()

            @pl.when(it == r * steps - 1)
            def _():
                for c in b_copies(r):
                    c.start()
                for c in w_copies(r) + b_copies(r):
                    c.wait()
        consume(it, it % 2)

        @pl.when(it >= (chips - 1) * steps)
        def _():
            out_copy(it % steps).start()
        produce(nxt, (it + 1) % 2)

    for i in range(steps):
        out_copy(i).wait()
    for m in range(3):
        for n in range(8):
            copy(m, n).wait_send()


def oproj_body(dims, meta, attn_ref, x_ref, gwo_ref, gb_ref, out_ref, wo, ao, bo, low, sems):
    n_dev, seqs, S, qw, rank, D, chips = dims
    n_ad = 2
    scale = ALPHA / rank
    step = pl.program_id(0)
    core = meta[seqs]
    per = seqs // chips
    steps = per // CORES
    plan = [(gwo_ref, wo)]
    for d in range(n_dev):
        for a in range(n_ad):
            plan.append((gb_ref.at[d, pl.ds(a * qw, qw)], ao.at[a, pl.ds(d * qw, qw)]))
            plan.append((gb_ref.at[d, pl.ds(n_ad * qw + a * rank, rank)], bo.at[a, :, pl.ds(d * qw, qw)]))

    @pl.when(step == 0)
    def _():
        for s, d in plan:
            pltpu.make_async_copy(s, d, sems.at[0]).start()
        for s, d in plan:
            pltpu.make_async_copy(s, d, sems.at[0]).wait()

    ids = [meta[t * per + core * steps + step] for t in range(chips)]
    for t in range(chips):
        low[pl.ds(t * S, S), :] = dot_nn(attn_ref[0, pl.ds(t * S, S), :], ao[ids[t]]).astype(BF16)
    nt = 256

    @pl.loop(0, D // nt)
    def _(j):
        cols = pl.ds(pl.multiple_of(j * nt, nt), nt)
        zo = dot_nn(attn_ref[0], wo[:, cols])
        for t in range(chips):
            z = zo[t * S:(t + 1) * S] + scale * dot_nn(low[pl.ds(t * S, S), :], bo[ids[t], :, cols])
            out_ref[t, 0, :, cols] = (x_ref[t, 0, :, cols].astype(F32) + z).astype(BF16)


def mlp_body(dims, ids_ref, x_ref, gain_ref, agu_ref, wg0, wg1, wu0, wu1, wd0, wd1, bg0, bg1, bu0, bu1, ad0, ad1, bd_ref,
             y_ref, wg, wu, wd, bg, bu, agu, ad, bd, xt, h_scr, low_scr, hid_scr, part, in_a, in_b, xo, ybuf,
             wsem, xsem, osem, sa, ra, sb, rb_, sy, ry, sf, rf, sp, rp):
    seqs, S, rank, D, chips = dims
    scale = ALPHA / rank
    fw = wg0.shape[1]
    per = seqs // chips
    steps = per // CORES
    M = chips * S
    hs = S // 2
    me = lax.axis_index('tensor')
    core, chip = me % CORES, me // CORES
    right_chip, left_chip = (chip + 1) % chips, (chip + chips - 1) % chips
    far_chip = (chip + 2) % chips
    right, left, other = right_chip * CORES + core, left_chip * CORES + core, chip * CORES + (1 - core)

    barrier = pltpu.get_barrier_semaphore()
    for dev in (right, left, other):
        pl.semaphore_signal(barrier, inc=1, device_id={'tensor': dev}, device_id_type=pl.DeviceIdType.MESH)
    pl.semaphore_wait(barrier, 3)

    def remote(src, dst, ssem, rsem, dev):
        return pltpu.make_async_remote_copy(src_ref=src, dst_ref=dst, send_sem=ssem, recv_sem=rsem,
                                            device_id={'tensor': dev}, device_id_type=pl.DeviceIdType.MESH)

    def copies_a(j):
        s, r = j % 3, j % 4
        return [remote(part.at[s, far_chip, pl.ds(0, hs)], in_a.at[0, r], sa.at[0, j], ra.at[0, j], right),
                remote(part.at[s, far_chip, pl.ds(hs, hs)], in_a.at[1, r], sa.at[1, j], ra.at[1, j], left)]

    def copies_b(j):
        s, r = j % 3, j % 3
        return [remote(part.at[s, right_chip], in_b.at[0, r], sb.at[0, j], rb_.at[0, j], right),
                remote(part.at[s, left_chip], in_b.at[1, r], sb.at[1, j], rb_.at[1, j], left)]

    def copies_y(j):
        dst = y_ref.at[me, j]
        src = ybuf.at[j % 2]
        return [remote(src, dst, sy.at[0, j], ry.at[0, j], right), remote(src, dst, sy.at[1, j], ry.at[1, j], left)]

    def copies_f(j):
        from_left = y_ref.at[left, j, pl.ds(0, hs)]
        from_right = y_ref.at[right, j, pl.ds(hs, hs)]
        return [remote(from_left, from_left, sf.at[0, j], rf.at[0, j], right),
                remote(from_right, from_right, sf.at[1, j], rf.at[1, j], left)]

    far = far_chip * CORES + core

    def copies_p(j):
        out = [remote(ybuf.at[j % 2], y_ref.at[me, j], sp.at[0, j], rp.at[0, j], other)]
        for n, dev in enumerate((left, right, far)):
            out.append(remote(y_ref.at[dev, j], y_ref.at[dev, j], sp.at[n + 1, j], rp.at[n + 1, j], other))
        return out

    def store_y(j):
        return pltpu.make_async_copy(ybuf.at[j % 2], y_ref.at[me, j], osem.at[j % 2])

    n_dev = chips * CORES
    rl = rank // n_dev
    ow = D // n_dev
    n_ad = agu.shape[0]
    plans = [[], [], []]
    for d in range(n_dev):
        for a in range(n_ad):
            for pr in range(2):
                plans[0].append((agu_ref.at[d, pl.ds((pr * n_ad + a) * rl, rl)], agu.at[a, pl.ds(pr * rank + d * rl, rl)]))
            plans[2].append((bd_ref.at[d, pl.ds(n_ad * (ow + rank) + a * rank, rank)], bd.at[a, :, pl.ds(d * ow, ow)]))
    for i, (g, u, b1, b2) in enumerate(((wg0, wu0, bg0, bu0), (wg1, wu1, bg1, bu1))):
        c = pl.ds(i * fw, fw)
        plans[1] += [(g, wg.at[:, c]), (u, wu.at[:, c]), (b1, bg.at[:, :, c]), (b2, bu.at[:, :, c])]
    for i, (d, a) in enumerate(((wd0, ad0), (wd1, ad1))):
        c = pl.ds(i * fw, fw)
        plans[2] += [(a, ad.at[:, c]), (d, wd.at[c])]
    n_plan = [0]
    flat = []
    for plan in plans:
        group = []
        for src, dst in plan:
            group.append(pltpu.make_async_copy(src, dst, wsem.at[n_plan[0]]))
            n_plan[0] += 1
        flat.append(group)

    def x_copy(i, slot):
        return pltpu.make_async_copy(x_ref.at[:, i], xt.at[slot], xsem.at[slot])

    def xo_copy(i):
        return pltpu.make_async_copy(x_ref.at[chip, i], xo.at[i % 2], xsem.at[2 + i % 2])

    x_copy(0, 0).start()
    for group in flat:
        for c in group:
            c.start()

    def arrive(i, step):
        @pl.when(step == 0)
        def _():
            for c in flat[i]:
                c.wait()

    nt = 256
    rb = 16

    def compute(k):
        slot = k % 2
        x_copy(k, slot).wait()

        @pl.when(k + 1 < steps)
        def _():
            x_copy(k + 1, 1 - slot).start()

        ids = [ids_ref[t * per + core * steps + k] for t in range(chips)]

        @pl.loop(0, M // rb)
        def _(i):
            t, r = i // (S // rb), i % (S // rb)
            v = xt[slot, t, pl.ds(pl.multiple_of(r * rb, rb), rb), :].astype(F32)
            inv = lax.rsqrt(jnp.mean(v * v, axis=-1, keepdims=True) + EPSILON)
            h_scr[pl.ds(pl.multiple_of(i * rb, rb), rb), :] = (v * inv * gain_ref[...]).astype(BF16)

        arrive(0, k)
        for t in range(chips):
            low_scr[pl.ds(t * S, S), :] = dot_nt(h_scr[pl.ds(t * S, S), :], agu[ids[t]]).astype(BF16)
        arrive(1, k)

        @pl.loop(0, wg.shape[1] // nt)
        def _(j):
            cols = pl.ds(pl.multiple_of(j * nt, nt), nt)
            zg = dot_nn(h_scr[...], wg[:, cols])
            zu = dot_nn(h_scr[...], wu[:, cols])
            for t in range(chips):
                rows = pl.ds(t * S, S)
                g = zg[t * S:(t + 1) * S] + scale * dot_nn(low_scr[rows, :rank], bg[ids[t], :, cols])
                u = zu[t * S:(t + 1) * S] + scale * dot_nn(low_scr[rows, rank:], bu[ids[t], :, cols])
                hid_scr[rows, cols] = (jax.nn.silu(g) * u).astype(BF16)

        arrive(2, k)

        @pl.when(k >= 3)
        def _():
            for c in copies_a(k - 3) + copies_b(k - 3):
                c.wait_send()
        s = k % 3
        for t in range(chips):
            part[s, t, :, D:] = dot_nn(hid_scr[pl.ds(t * S, S), :], ad[ids[t]]).astype(BF16)

        @pl.loop(0, D // nt)
        def _(j):
            cols = pl.ds(pl.multiple_of(j * nt, nt), nt)
            z = dot_nn(hid_scr[...], wd[:, cols])
            for t in range(chips):
                part[s, t, :, cols] = z[t * S:(t + 1) * S].astype(BF16)

        for c in copies_a(k):
            c.start()

    def relay(j):
        s, r = j % 3, j % 4
        for n, (dest, lo) in enumerate(((right_chip, 0), (left_chip, hs))):
            copies_a(j)[n].wait_recv()

            @pl.loop(0, hs // rb)
            def _(i):
                rows = pl.ds(pl.multiple_of(lo + i * rb, rb), rb)
                got = in_a[n, r, pl.ds(pl.multiple_of(i * rb, rb), rb), :]
                part[s, dest, rows, :] = (part[s, dest, rows, :].astype(F32) + got.astype(F32)).astype(BF16)
            copies_b(j)[n].start()
        xo_copy(j).start()

    def settle(j):
        s = j % 3
        for c in copies_b(j):
            c.wait_recv()
        xo_copy(j).wait()

        @pl.when(j >= 2)
        def _():
            store_y(j - 2).wait()
            for c in copies_y(j - 2) + copies_p(j - 2)[:1]:
                c.wait_send()
        idx = ids_ref[chip * per + core * steps + j]

        def total(cols):
            return (part[s, chip, :, cols].astype(F32) + in_b[0, s, :, cols].astype(F32)) + in_b[1, s, :, cols].astype(F32)

        low = total(pl.ds(D, rank)).astype(BF16)

        @pl.loop(0, D // nt)
        def _(i):
            cols = pl.ds(pl.multiple_of(i * nt, nt), nt)
            z = total(cols) + scale * dot_nn(low, bd[idx, :, cols])
            ybuf[j % 2, :, cols] = (xo[j % 2, :, cols].astype(F32) + z).astype(BF16)
        store_y(j).start()
        for c in copies_y(j) + copies_p(j)[:1]:
            c.start()

    def forward(j):
        for n in range(2):
            copies_y(j)[n].wait_recv()
            copies_f(j)[n].start()
            copies_p(j)[1 + n].start()

    def last_hop(j):
        for c in copies_f(j):
            c.wait_recv()
        copies_p(j)[3].start()

    @pl.loop(0, steps + 4)
    def _(k):
        @pl.when(k < steps)
        def _():
            compute(k)
        for lag, stage in ((1, relay), (2, settle), (3, forward), (4, last_hop)):
            @pl.when((k >= lag) & (k < steps + lag))
            def _():
                stage(k - lag)

    for j in range(max(0, steps - 3), steps):
        for c in copies_a(j) + copies_b(j):
            c.wait_send()
    for j in range(max(0, steps - 2), steps):
        store_y(j).wait()
        for c in copies_y(j) + copies_p(j)[:1]:
            c.wait_send()

    @pl.loop(0, steps)
    def _(j):
        for c in copies_f(j) + copies_p(j)[1:]:
            c.wait_send()
        for c in copies_p(j):
            c.wait_recv()


def solution(mesh):
    n_dev = mesh.shape['tensor']
    chips = n_dev // CORES
    head_split = P(None, 'tensor', None)
    last_split = P(None, None, 'tensor')
    b_head_split = P(None, None, 'tensor', None)
    in_specs = (P('data', None, None), P('data'), P(None), P(None),
                head_split, head_split, head_split, P('tensor', None, None),
                P(None, 'tensor'), P(None, 'tensor'), P('tensor', None),
                last_split, b_head_split, last_split, b_head_split, last_split, b_head_split,
                P(None, 'tensor', None, None), last_split,
                last_split, last_split, last_split, last_split,
                P(None, 'tensor', None), last_split)
    swap = [(i, i ^ 1) for i in range(n_dev)]
    ANY = pl.BlockSpec(memory_space=pl.ANY)

    def local_layer(x_in, adapter_ids, gain_attn, gain_mlp, w_q, w_k, w_v, w_o, w_gate, w_up, w_down, a_q, b_q, a_k, b_k, a_v, b_v, a_o, b_o, a_gate, b_gate, a_up, b_up, a_down, b_down):
        seqs, S, D = x_in.shape
        nq, hd = w_q.shape[1], w_q.shape[2]
        n_ad, rank = b_q.shape[0], b_q.shape[1]
        rl = a_q.shape[2]
        half = hd // 2
        qw = nq * hd
        per = seqs // chips
        steps = per // CORES

        def rows_t(w):
            return jnp.transpose(w, (1, 2, 0)).reshape(-1, w.shape[0])

        gather = functools.partial(lax.all_gather, axis_name='tensor', axis=0)
        swapped = functools.partial(lax.ppermute, axis_name='tensor', perm=swap)

        def rows_a(stacks):
            return jnp.concatenate([jnp.transpose(a, (0, 2, 1)).reshape(n_ad * rl, D) for a in stacks], axis=0)

        def b_rows(b):
            return jnp.transpose(b, (1, 2, 0)).reshape(-1, rank)

        a_own = rows_a((a_q, a_k, a_v))
        w_own = jnp.concatenate([rows_t(w_q), rows_t(w_k), rows_t(w_v)], axis=0)
        b_own = jnp.concatenate([b_rows(b[a]) for a in range(n_ad) for b in (b_q, b_k, b_v)], axis=0)
        g_wo = gather(w_o.reshape(qw, D))
        g_b = gather(jnp.concatenate([a_o.reshape(n_ad * qw, rank), b_o.reshape(n_ad * rank, qw),
                                      b_down.reshape(n_ad * rank, qw)], axis=0))
        g_gu = gather(rows_a((a_gate, a_up)))
        mlp_own = (w_gate, w_up, w_down, b_gate, b_up, a_down)
        mlp_other = tuple(swapped(w) for w in mlp_own)

        inv_freq = ROPE_BASE ** (-2.0 * jnp.arange(half, dtype=F32) / hd)
        ang = jnp.arange(S, dtype=F32)[:, None] * inv_freq[None, :]
        cos, sin = jnp.cos(ang), jnp.sin(ang)
        cos_t, sin_t = cos.T, sin.T

        x4 = x_in.reshape(chips, per, S, D)
        M = chips * S
        Fc = CORES * w_gate.shape[1]
        dma = pltpu.SemaphoreType.DMA
        dw = qw + 2 * hd
        attn_all = pl.pallas_call(
            functools.partial(attn_body, (n_dev, seqs, S, hd, nq, rank, D, chips)),
            in_specs=[pl.BlockSpec(memory_space=pltpu.SMEM), ANY] + [pl.BlockSpec(memory_space=pltpu.VMEM)] * 3 + [ANY] * 3,
            out_specs=[ANY] * 4,
            scratch_shapes=[
                pltpu.VMEM((steps, D, M), BF16), pltpu.VMEM((steps, 3 * rank, M), BF16), pltpu.VMEM((steps, M, n_dev * qw), BF16),
                pltpu.VMEM((chips, CORES * dw, D), BF16), pltpu.VMEM((chips, n_ad, CORES * dw, rank), BF16),
                pltpu.VMEM((2, CORES * qw, M), BF16), pltpu.VMEM((2, CORES, M, hd), BF16), pltpu.VMEM((2, CORES * hd, M), BF16),
                dma((n_dev, 3 * n_ad)), dma((chips, CORES, 1 + n_ad)), dma((2, chips)), dma((steps,)), dma((3, 8)), dma((3, 8))],
            out_shape=[jax.ShapeDtypeStruct((steps, M, n_dev * qw), BF16), jax.ShapeDtypeStruct((n_dev,) + a_own.shape, BF16),
                       jax.ShapeDtypeStruct((n_dev,) + w_own.shape, BF16), jax.ShapeDtypeStruct((n_dev,) + b_own.shape, BF16)],
            compiler_params=pltpu.CompilerParams(vmem_limit_bytes=VMEM_LIMIT, collective_id=1, has_side_effects=True),
            name="attn_ring",
            cost_estimate=pl.CostEstimate(flops=3 * steps * M * D * (n_dev * qw + 2 * n_dev * hd + 3 * rank),
                                          bytes_accessed=6 * steps * M * D + 33 * 2**20, transcendentals=0),
        )(adapter_ids, x4, gain_attn.reshape(1, D), cos_t, sin_t, a_own, w_own, b_own)[0]
        core = lax.axis_index('tensor') % CORES
        meta = jnp.concatenate([adapter_ids.astype(jnp.int32), core.reshape(1).astype(jnp.int32)])
        x1_all = pl.pallas_call(
            functools.partial(oproj_body, (n_dev, seqs, S, qw, rank, D, chips)),
            grid_spec=pltpu.PrefetchScalarGridSpec(
                num_scalar_prefetch=1, grid=(steps,),
                in_specs=[pl.BlockSpec((1, M, n_dev * qw), lambda i, m: (i, 0, 0)),
                          pl.BlockSpec((chips, 1, S, D), lambda i, m: (0, m[seqs] * steps + i, 0, 0)), ANY, ANY],
                out_specs=pl.BlockSpec((chips, 1, S, D), lambda i, m: (0, i, 0, 0)),
                scratch_shapes=[pltpu.VMEM((n_dev * qw, D), BF16), pltpu.VMEM((n_ad, n_dev * qw, rank), BF16),
                                pltpu.VMEM((n_ad, rank, D), BF16), pltpu.VMEM((M, rank), BF16), dma((1,))]),
            out_shape=jax.ShapeDtypeStruct((chips, steps, S, D), BF16),
            compiler_params=pltpu.CompilerParams(vmem_limit_bytes=VMEM_LIMIT, dimension_semantics=("arbitrary",)), name="oproj",
            cost_estimate=pl.CostEstimate(flops=2 * steps * M * D * (D + 2 * rank),
                                          bytes_accessed=6 * steps * M * D + 12 * 2**20, transcendentals=0),
        )(meta, attn_all, x4, g_wo.reshape(n_dev * qw, D), g_b)
        pairs = [w for own, other in zip(mlp_own, mlp_other) for w in (own, other)]
        y = pl.pallas_call(
            functools.partial(mlp_body, (seqs, S, rank, D, chips)),
            in_specs=[pl.BlockSpec(memory_space=pltpu.SMEM), ANY, pl.BlockSpec(memory_space=pltpu.VMEM)] + [ANY] * 14,
            out_specs=ANY,
            scratch_shapes=[
                pltpu.VMEM((D, Fc), BF16), pltpu.VMEM((D, Fc), BF16), pltpu.VMEM((Fc, D), BF16),
                pltpu.VMEM((n_ad, rank, Fc), BF16), pltpu.VMEM((n_ad, rank, Fc), BF16),
                pltpu.VMEM((n_ad, 2 * rank, D), BF16), pltpu.VMEM((n_ad, Fc, rank), BF16), pltpu.VMEM((n_ad, rank, D), BF16),
                pltpu.VMEM((2, chips, S, D), BF16), pltpu.VMEM((M, D), BF16), pltpu.VMEM((M, 2 * rank), BF16), pltpu.VMEM((M, Fc), BF16),
                pltpu.VMEM((3, chips, S, D + rank), BF16), pltpu.VMEM((2, 4, S // 2, D + rank), BF16),
                pltpu.VMEM((2, 3, S, D + rank), BF16), pltpu.VMEM((2, S, D), BF16), pltpu.VMEM((2, S, D), BF16),
                dma((12 + n_dev * n_ad * 3,)), dma((4,)), dma((2,)), dma((2, steps)), dma((2, steps)), dma((2, steps)), dma((2, steps)),
                dma((2, steps)), dma((2, steps)), dma((2, steps)), dma((2, steps)), dma((4, steps)), dma((4, steps))],
            out_shape=jax.ShapeDtypeStruct((n_dev, steps, S, D), BF16),
            compiler_params=pltpu.CompilerParams(vmem_limit_bytes=VMEM_LIMIT, collective_id=0, has_side_effects=True),
            name="mlp_ring",
            cost_estimate=pl.CostEstimate(flops=2 * steps * M * D * (3 * Fc + 4 * rank),
                                          bytes_accessed=8 * steps * M * D + 34 * 2**20, transcendentals=steps * M * Fc),
        )(adapter_ids, x1_all, gain_mlp.reshape(1, D), g_gu, *pairs, g_b)
        return y.reshape(seqs, S, D)

    return jax.shard_map(local_layer, mesh=mesh, in_specs=in_specs, out_specs=P('data', None, None), check_vma=False)
```

```python
import functools

import jax
import jax.numpy as jnp
from jax import lax
from jax.experimental import pallas as pl
from jax.experimental.pallas import tpu as pltpu
from jax.sharding import PartitionSpec as P

ALPHA = 16.0
ROPE_BASE = 10000.0
EPSILON = 1e-5
CORES = 2
VMEM_LIMIT = 62 * 1024 * 1024
F32, BF16 = jnp.float32, jnp.bfloat16


def dot_nn(a, b):
    return lax.dot_general(a, b, (((1,), (0,)), ((), ())), preferred_element_type=F32)


def dot_nt(a, b):
    return lax.dot_general(a, b, (((1,), (1,)), ((), ())), preferred_element_type=F32)


def attn_body(dims, ids_ref, x_ref, gain_ref, cos_ref, sin_ref, a_own, w_own, b_own, o_own, l_own, u_own,
              out_ref, ga, gw, gb, go, gl, gu,
              h, low, attn, w, bw, q_scr, k_scr, v_scr, asem, wsem, xsem, osem, ss, rs):
    n_dev, seqs, S, hd, nq, rank, D, chips = dims
    half = hd // 2
    qw = nq * hd
    n_ad = 2
    scale = ALPHA / rank
    me = lax.axis_index('tensor')
    core, chip = me % CORES, me // CORES
    per = seqs // chips
    steps = per // CORES
    M = chips * S
    dw = qw + 2 * hd
    rl = rank // n_dev
    right_chip, left_chip, far_chip = (chip + 1) % chips, (chip + chips - 1) % chips, (chip + 2) % chips
    order = [(chip + r) % chips for r in range(chips)]
    right, left, far = [c * CORES + core for c in (right_chip, left_chip, far_chip)]
    other = chip * CORES + (1 - core)

    barrier = pltpu.get_barrier_semaphore()
    for dev in (right, left, other):
        pl.semaphore_signal(barrier, inc=1, device_id={'tensor': dev}, device_id_type=pl.DeviceIdType.MESH)
    pl.semaphore_wait(barrier, 3)

    groups = ((a_own, ga), (w_own, gw), (b_own, gb), (o_own, go), (l_own, gl), (u_own, gu))
    now, later = (1, 2), (3, 4, 5)

    def remote(m, n, src, dst, dev):
        return pltpu.make_async_remote_copy(src_ref=src, dst_ref=dst, send_sem=ss.at[m, n], recv_sem=rs.at[m, n],
                                            device_id={'tensor': dev}, device_id_type=pl.DeviceIdType.MESH)

    def copy(m, n):
        own, buf = groups[m]
        n_rows = own.shape[0] // 2
        if n == 0:
            return remote(m, n, own, buf.at[me], right)
        if n == 1:
            return remote(m, n, own, buf.at[me], left)
        if n == 2:
            part = buf.at[left, pl.ds(0, n_rows)]
            return remote(m, n, part, part, right)
        if n == 3:
            part = buf.at[right, pl.ds(n_rows, n_rows)]
            return remote(m, n, part, part, left)
        if n == 4:
            return remote(m, n, own, buf.at[me], other)
        dev = (left, right, far)[n - 5]
        return remote(m, n, buf.at[dev], buf.at[dev], other)

    def send_own(m):
        for n in (0, 1, 4):
            copy(m, n).start()

    def pass_on(m):
        for n in (0, 1):
            copy(m, n).wait_recv()
            copy(m, 2 + n).start()
            copy(m, 5 + n).start()

    def pass_far(m):
        for n in (2, 3):
            copy(m, n).wait_recv()
        copy(m, 7).start()

    def seq_id(i, t):
        return ids_ref[t * per + core * steps + i]

    x_base = 4

    def a_copies(dev, src, n):
        out = []
        for pr in range(3):
            for a in range(n_ad):
                k = pr * n_ad + a
                o = pl.multiple_of(dev * rl, rl)
                dst = attn.at[a, pl.ds(pr * rank + o, rl)] if pr < 2 else attn.at[n_ad + a, pl.ds(o, rl)]
                out.append(pltpu.make_async_copy(src.at[pl.ds(k * rl, rl)], dst, asem.at[n, k]))
        return out

    def w_copies(r):
        out = []
        for n, c in enumerate((core, 1 - core)):
            src = w_own if r == 0 and n == 0 else gw.at[order[r] * CORES + c]
            out.append(pltpu.make_async_copy(src, w.at[r, pl.ds(pl.multiple_of(c * dw, dw), dw)], wsem.at[r, n, 0]))
        return out

    def b_copies(r):
        out = []
        for n, c in enumerate((core, 1 - core)):
            src = b_own if r == 0 and n == 0 else gb.at[order[r] * CORES + c]
            for a in range(n_ad):
                out.append(pltpu.make_async_copy(src.at[pl.ds(a * dw, dw)],
                                                 bw.at[r, a, pl.ds(pl.multiple_of(c * dw, dw), dw)], wsem.at[r, n, 1 + a]))
        return out

    def x_copies(i, slot):
        return [pltpu.make_async_copy(x_ref.at[t, core * steps + i],
                                      attn.at[x_base + slot, pl.ds(t * S, S)], xsem.at[slot, t])
                for t in range(chips)]

    send_own(0)
    for c in x_copies(0, 0):
        c.start()
    rb = 16

    @pl.loop(0, steps)
    def _(i):
        slot = i % 2
        for c in x_copies(i, slot):
            c.wait()

        @pl.when(i + 1 < steps)
        def _():
            for c in x_copies(i + 1, 1 - slot):
                c.start()

        @pl.loop(0, M // rb)
        def _(r):
            v = attn[x_base + slot, pl.ds(pl.multiple_of(r * rb, rb), rb), :].astype(F32)
            inv = lax.rsqrt(jnp.mean(v * v, axis=-1, keepdims=True) + EPSILON)
            attn[x_base + 2, pl.ds(pl.multiple_of(r * rb, rb), rb), :] = (v * inv * gain_ref[...]).astype(BF16)

        @pl.loop(0, D // S)
        def _(c):
            block = pl.ds(pl.multiple_of(c * S, S), S)
            h[i, block, :] = attn[x_base + 2, :, block].T

    pass_on(0)
    send_own(1)
    send_own(2)
    devs = [order[r] * CORES + c for r in range(chips) for c in (core, 1 - core)]
    pass_far(0)
    for n in range(4):
        copy(0, 4 + n).wait_recv()
    stacks = [c for n, dev in enumerate(devs) for c in a_copies(dev, a_own if n == 0 else ga.at[dev], n)]
    for c in stacks:
        c.start()
    for c in stacks:
        c.wait()

    @pl.loop(0, steps)
    def _(i):
        for t in range(chips):
            idx = seq_id(i, t)
            cols = slice(t * S, (t + 1) * S)
            low[i, :2 * rank, cols] = dot_nn(attn[idx], h[i, :, cols]).astype(BF16)
            low[i, 2 * rank:, cols] = dot_nn(attn[n_ad + idx, :rank], h[i, :, cols]).astype(BF16)

    def produce(it, slot):
        r, i = it // steps, it % steps
        z = dot_nn(w[r], h[i])
        for t in range(chips):
            b = bw[r, seq_id(i, t)]
            cols = slice(t * S, (t + 1) * S)

            def project(o, n, c0):
                zz = jnp.concatenate([z[c * dw + o:c * dw + o + n, cols] for c in range(CORES)], axis=0)
                bb = jnp.concatenate([b[c * dw + o:c * dw + o + n] for c in range(CORES)], axis=0)
                return zz + scale * dot_nn(bb, low[i, c0:c0 + rank, cols])

            zq, zk, zv = project(0, qw, 0), project(qw, hd, rank), project(qw + hd, hd, 2 * rank)
            cos, sin = cos_ref[...], sin_ref[...]

            def rotate(v):
                f, s = v[:half], v[half:]
                return jnp.concatenate([f * cos - s * sin, s * cos + f * sin], axis=0)

            for hh in range(CORES * nq):
                o = hh * hd
                q_scr[slot, o:o + hd, cols] = (rotate(zq[o:o + hd]) * hd ** -0.5).astype(BF16)
            kt = jnp.concatenate([rotate(zk[c * hd:(c + 1) * hd]) for c in range(CORES)], axis=0)
            kk = kt.T.astype(BF16)
            for c in range(CORES):
                k_scr[slot, c, t * S:(t + 1) * S, :] = kk[:, c * hd:(c + 1) * hd]
            v_scr[slot, :, cols] = zv.astype(BF16)

    def consume(it, slot):
        r, i = it // steps, it % steps
        p = (chip + r) % chips
        key = lax.broadcasted_iota(jnp.int32, (S, S), 0)
        qry = lax.broadcasted_iota(jnp.int32, (S, S), 1)
        causal = key <= qry
        for c in range(CORES):
            for t in range(chips):
                cols = slice(t * S, (t + 1) * S)
                q = jnp.concatenate([q_scr[slot, c * qw + hh * hd:c * qw + (hh + 1) * hd, cols] for hh in range(nq)], axis=1)
                sc = dot_nn(k_scr[slot, c, cols, :], q)
                ps = []
                for hh in range(nq):
                    sh = jnp.where(causal, sc[:, hh * S:(hh + 1) * S], -1e30)
                    e = jnp.exp(sh - jnp.max(sh, axis=0, keepdims=True))
                    ps.append((e * (1.0 / jnp.sum(e, axis=0, keepdims=True))).astype(BF16))
                o = dot_nn(v_scr[slot, c * hd:(c + 1) * hd, cols], jnp.concatenate(ps, axis=1))
                o = jnp.concatenate([o[:, hh * S:(hh + 1) * S] for hh in range(nq)], axis=0)
                attn[i, pl.ds(t * S, S),
                     pl.ds(pl.multiple_of((p * CORES + c) * qw, qw), qw)] = o.T.astype(BF16)

    def out_copy(i):
        return pltpu.make_async_copy(attn.at[i], out_ref.at[i], osem.at[i])

    for m in (1, 2):
        copy(m, 4).wait_recv()
    for c in w_copies(0) + b_copies(0):
        c.start()
    for c in w_copies(0) + b_copies(0):
        c.wait()
    produce(0, 0)

    @pl.loop(0, chips * steps)
    def _(it):
        nxt = jnp.minimum(it + 1, chips * steps - 1)

        @pl.when(it == 2)
        def _():
            for m in now:
                pass_on(m)
            for m in later:
                send_own(m)

        @pl.when(it == steps)
        def _():
            for m in now:
                pass_far(m)

        @pl.when(it == 2 * steps + 2)
        def _():
            for m in later:
                pass_on(m)

        @pl.when(it == 3 * steps + 3)
        def _():
            for m in later:
                pass_far(m)
        for r in range(1, chips):
            @pl.when(it == r * steps - 2)
            def _():
                for m in (1, 2):
                    copy(m, (4, 6, 7, 5)[r]).wait_recv()
                for c in w_copies(r):
                    c.start()

            @pl.when(it == r * steps - 1)
            def _():
                for c in b_copies(r):
                    c.start()
                for c in w_copies(r) + b_copies(r):
                    c.wait()
        consume(it, it % 2)

        @pl.when(it >= (chips - 1) * steps)
        def _():
            out_copy(it % steps).start()
        produce(nxt, (it + 1) % 2)

    for i in range(steps):
        out_copy(i).wait()
    for m in later:
        for n in range(4):
            copy(m, 4 + n).wait_recv()
    for m in range(len(groups)):
        for n in range(8):
            copy(m, n).wait_send()


def oproj_body(dims, meta, attn_ref, x_ref, gwo_ref, gb_ref, out_ref, wo, ao, bo, low, sems):
    n_dev, seqs, S, qw, rank, D, chips = dims
    n_ad = 2
    scale = ALPHA / rank
    step = pl.program_id(0)
    core = meta[seqs]
    per = seqs // chips
    steps = per // CORES
    plan = [(gwo_ref, wo)]
    for d in range(n_dev):
        for a in range(n_ad):
            plan.append((gb_ref.at[d, pl.ds(a * qw, qw)], ao.at[a, pl.ds(d * qw, qw)]))
            plan.append((gb_ref.at[d, pl.ds(n_ad * qw + a * rank, rank)], bo.at[a, :, pl.ds(d * qw, qw)]))

    @pl.when(step == 0)
    def _():
        for s, d in plan:
            pltpu.make_async_copy(s, d, sems.at[0]).start()
        for s, d in plan:
            pltpu.make_async_copy(s, d, sems.at[0]).wait()

    ids = [meta[t * per + core * steps + step] for t in range(chips)]
    for t in range(chips):
        low[pl.ds(t * S, S), :] = dot_nn(attn_ref[0, pl.ds(t * S, S), :], ao[ids[t]]).astype(BF16)
    nt = 256

    @pl.loop(0, D // nt)
    def _(j):
        cols = pl.ds(pl.multiple_of(j * nt, nt), nt)
        zo = dot_nn(attn_ref[0], wo[:, cols])
        for t in range(chips):
            z = zo[t * S:(t + 1) * S] + scale * dot_nn(low[pl.ds(t * S, S), :], bo[ids[t], :, cols])
            out_ref[t, 0, :, cols] = (x_ref[t, 0, :, cols].astype(F32) + z).astype(BF16)


def mlp_body(dims, ids_ref, x_ref, gain_ref, agu_ref, wg0, wg1, wu0, wu1, wd0, wd1, bg0, bg1, bu0, bu1, ad0, ad1, bd_ref,
             y_ref, wg, wu, wd, bg, bu, agu, ad, bd, xt, h_scr, low_scr, hid_scr, part, in_a, in_b, xo, ybuf,
             wsem, xsem, osem, sa, ra, sb, rb_, sy, ry, sf, rf, sp, rp):
    seqs, S, rank, D, chips = dims
    scale = ALPHA / rank
    fw = wg0.shape[1]
    per = seqs // chips
    steps = per // CORES
    M = chips * S
    hs = S // 2
    me = lax.axis_index('tensor')
    core, chip = me % CORES, me // CORES
    right_chip, left_chip = (chip + 1) % chips, (chip + chips - 1) % chips
    far_chip = (chip + 2) % chips
    right, left, other = right_chip * CORES + core, left_chip * CORES + core, chip * CORES + (1 - core)

    barrier = pltpu.get_barrier_semaphore()
    for dev in (right, left, other):
        pl.semaphore_signal(barrier, inc=1, device_id={'tensor': dev}, device_id_type=pl.DeviceIdType.MESH)
    pl.semaphore_wait(barrier, 3)

    def remote(src, dst, ssem, rsem, dev):
        return pltpu.make_async_remote_copy(src_ref=src, dst_ref=dst, send_sem=ssem, recv_sem=rsem,
                                            device_id={'tensor': dev}, device_id_type=pl.DeviceIdType.MESH)

    def copies_a(j):
        s, r = j % 3, j % 4
        return [remote(part.at[s, far_chip, pl.ds(0, hs)], in_a.at[0, r], sa.at[0, j], ra.at[0, j], right),
                remote(part.at[s, far_chip, pl.ds(hs, hs)], in_a.at[1, r], sa.at[1, j], ra.at[1, j], left)]

    def copies_b(j):
        s, r = j % 3, j % 3
        return [remote(part.at[s, right_chip], in_b.at[0, r], sb.at[0, j], rb_.at[0, j], right),
                remote(part.at[s, left_chip], in_b.at[1, r], sb.at[1, j], rb_.at[1, j], left)]

    def copies_y(j):
        dst = y_ref.at[me, j]
        src = ybuf.at[j % 2]
        return [remote(src, dst, sy.at[0, j], ry.at[0, j], right), remote(src, dst, sy.at[1, j], ry.at[1, j], left)]

    def copies_f(j):
        from_left = y_ref.at[left, j, pl.ds(0, hs)]
        from_right = y_ref.at[right, j, pl.ds(hs, hs)]
        return [remote(from_left, from_left, sf.at[0, j], rf.at[0, j], right),
                remote(from_right, from_right, sf.at[1, j], rf.at[1, j], left)]

    far = far_chip * CORES + core

    def copies_p(j):
        out = [remote(ybuf.at[j % 2], y_ref.at[me, j], sp.at[0, j], rp.at[0, j], other)]
        for n, dev in enumerate((left, right, far)):
            out.append(remote(y_ref.at[dev, j], y_ref.at[dev, j], sp.at[n + 1, j], rp.at[n + 1, j], other))
        return out

    def store_y(j):
        return pltpu.make_async_copy(ybuf.at[j % 2], y_ref.at[me, j], osem.at[j % 2])

    n_dev = chips * CORES
    rl = rank // n_dev
    ow = D // n_dev
    n_ad = agu.shape[0]
    plans = [[], [], []]
    for d in range(n_dev):
        for a in range(n_ad):
            for pr in range(2):
                plans[0].append((agu_ref.at[d, pl.ds((pr * n_ad + a) * rl, rl)], agu.at[a, pl.ds(pr * rank + d * rl, rl)]))
            plans[2].append((bd_ref.at[d, pl.ds(n_ad * (ow + rank) + a * rank, rank)], bd.at[a, :, pl.ds(d * ow, ow)]))
    for i, (g, u, b1, b2) in enumerate(((wg0, wu0, bg0, bu0), (wg1, wu1, bg1, bu1))):
        c = pl.ds(i * fw, fw)
        plans[1] += [(g, wg.at[:, c]), (u, wu.at[:, c]), (b1, bg.at[:, :, c]), (b2, bu.at[:, :, c])]
    for i, (d, a) in enumerate(((wd0, ad0), (wd1, ad1))):
        c = pl.ds(i * fw, fw)
        plans[2] += [(a, ad.at[:, c]), (d, wd.at[c])]
    n_plan = [0]
    flat = []
    for plan in plans:
        group = []
        for src, dst in plan:
            group.append(pltpu.make_async_copy(src, dst, wsem.at[n_plan[0]]))
            n_plan[0] += 1
        flat.append(group)

    def x_copy(i, slot):
        return pltpu.make_async_copy(x_ref.at[:, i], xt.at[slot], xsem.at[slot])

    def xo_copy(i):
        return pltpu.make_async_copy(x_ref.at[chip, i], xo.at[i % 2], xsem.at[2 + i % 2])

    x_copy(0, 0).start()
    for group in flat:
        for c in group:
            c.start()

    def arrive(i, step):
        @pl.when(step == 0)
        def _():
            for c in flat[i]:
                c.wait()

    nt = 256
    rb = 16

    def compute(k):
        slot = k % 2
        x_copy(k, slot).wait()

        @pl.when(k + 1 < steps)
        def _():
            x_copy(k + 1, 1 - slot).start()

        ids = [ids_ref[t * per + core * steps + k] for t in range(chips)]

        @pl.loop(0, M // rb)
        def _(i):
            t, r = i // (S // rb), i % (S // rb)
            v = xt[slot, t, pl.ds(pl.multiple_of(r * rb, rb), rb), :].astype(F32)
            inv = lax.rsqrt(jnp.mean(v * v, axis=-1, keepdims=True) + EPSILON)
            h_scr[pl.ds(pl.multiple_of(i * rb, rb), rb), :] = (v * inv * gain_ref[...]).astype(BF16)

        arrive(0, k)
        for t in range(chips):
            low_scr[pl.ds(t * S, S), :] = dot_nt(h_scr[pl.ds(t * S, S), :], agu[ids[t]]).astype(BF16)
        arrive(1, k)

        @pl.loop(0, wg.shape[1] // nt)
        def _(j):
            cols = pl.ds(pl.multiple_of(j * nt, nt), nt)
            zg = dot_nn(h_scr[...], wg[:, cols])
            zu = dot_nn(h_scr[...], wu[:, cols])
            for t in range(chips):
                rows = pl.ds(t * S, S)
                g = zg[t * S:(t + 1) * S] + scale * dot_nn(low_scr[rows, :rank], bg[ids[t], :, cols])
                u = zu[t * S:(t + 1) * S] + scale * dot_nn(low_scr[rows, rank:], bu[ids[t], :, cols])
                hid_scr[rows, cols] = (jax.nn.silu(g) * u).astype(BF16)

        arrive(2, k)

        @pl.when(k >= 3)
        def _():
            for c in copies_a(k - 3) + copies_b(k - 3):
                c.wait_send()
        s = k % 3
        for t in range(chips):
            part[s, t, :, D:] = dot_nn(hid_scr[pl.ds(t * S, S), :], ad[ids[t]]).astype(BF16)

        @pl.loop(0, D // nt)
        def _(j):
            cols = pl.ds(pl.multiple_of(j * nt, nt), nt)
            z = dot_nn(hid_scr[...], wd[:, cols])
            for t in range(chips):
                part[s, t, :, cols] = z[t * S:(t + 1) * S].astype(BF16)

        for c in copies_a(k):
            c.start()

    def relay(j):
        s, r = j % 3, j % 4
        for n, (dest, lo) in enumerate(((right_chip, 0), (left_chip, hs))):
            copies_a(j)[n].wait_recv()

            @pl.loop(0, hs // rb)
            def _(i):
                rows = pl.ds(pl.multiple_of(lo + i * rb, rb), rb)
                got = in_a[n, r, pl.ds(pl.multiple_of(i * rb, rb), rb), :]
                part[s, dest, rows, :] = (part[s, dest, rows, :].astype(F32) + got.astype(F32)).astype(BF16)
            copies_b(j)[n].start()
        xo_copy(j).start()

    def settle(j):
        s = j % 3
        for c in copies_b(j):
            c.wait_recv()
        xo_copy(j).wait()

        @pl.when(j >= 2)
        def _():
            store_y(j - 2).wait()
            for c in copies_y(j - 2) + copies_p(j - 2)[:1]:
                c.wait_send()
        idx = ids_ref[chip * per + core * steps + j]

        def total(cols):
            return (part[s, chip, :, cols].astype(F32) + in_b[0, s, :, cols].astype(F32)) + in_b[1, s, :, cols].astype(F32)

        low = total(pl.ds(D, rank)).astype(BF16)

        @pl.loop(0, D // nt)
        def _(i):
            cols = pl.ds(pl.multiple_of(i * nt, nt), nt)
            z = total(cols) + scale * dot_nn(low, bd[idx, :, cols])
            ybuf[j % 2, :, cols] = (xo[j % 2, :, cols].astype(F32) + z).astype(BF16)
        store_y(j).start()
        for c in copies_y(j) + copies_p(j)[:1]:
            c.start()

    def forward(j):
        for n in range(2):
            copies_y(j)[n].wait_recv()
            copies_f(j)[n].start()
            copies_p(j)[1 + n].start()

    def last_hop(j):
        for c in copies_f(j):
            c.wait_recv()
        copies_p(j)[3].start()

    @pl.loop(0, steps + 4)
    def _(k):
        @pl.when(k < steps)
        def _():
            compute(k)
        for lag, stage in ((1, relay), (2, settle), (3, forward), (4, last_hop)):
            @pl.when((k >= lag) & (k < steps + lag))
            def _():
                stage(k - lag)

    for j in range(max(0, steps - 3), steps):
        for c in copies_a(j) + copies_b(j):
            c.wait_send()
    for j in range(max(0, steps - 2), steps):
        store_y(j).wait()
        for c in copies_y(j) + copies_p(j)[:1]:
            c.wait_send()

    @pl.loop(0, steps)
    def _(j):
        for c in copies_f(j) + copies_p(j)[1:]:
            c.wait_send()
        for c in copies_p(j):
            c.wait_recv()


def solution(mesh):
    n_dev = mesh.shape['tensor']
    chips = n_dev // CORES
    head_split = P(None, 'tensor', None)
    last_split = P(None, None, 'tensor')
    b_head_split = P(None, None, 'tensor', None)
    in_specs = (P('data', None, None), P('data'), P(None), P(None),
                head_split, head_split, head_split, P('tensor', None, None),
                P(None, 'tensor'), P(None, 'tensor'), P('tensor', None),
                last_split, b_head_split, last_split, b_head_split, last_split, b_head_split,
                P(None, 'tensor', None, None), last_split,
                last_split, last_split, last_split, last_split,
                P(None, 'tensor', None), last_split)
    swap = [(i, i ^ 1) for i in range(n_dev)]
    ANY = pl.BlockSpec(memory_space=pl.ANY)

    def local_layer(x_in, adapter_ids, gain_attn, gain_mlp, w_q, w_k, w_v, w_o, w_gate, w_up, w_down, a_q, b_q, a_k, b_k, a_v, b_v, a_o, b_o, a_gate, b_gate, a_up, b_up, a_down, b_down):
        seqs, S, D = x_in.shape
        nq, hd = w_q.shape[1], w_q.shape[2]
        n_ad, rank = b_q.shape[0], b_q.shape[1]
        rl = a_q.shape[2]
        half = hd // 2
        qw = nq * hd
        per = seqs // chips
        steps = per // CORES

        def rows_t(w):
            return jnp.transpose(w, (1, 2, 0)).reshape(-1, w.shape[0])

        swapped = functools.partial(lax.ppermute, axis_name='tensor', perm=swap)

        def rows_a(stacks):
            return jnp.concatenate([jnp.transpose(a, (0, 2, 1)).reshape(n_ad * rl, D) for a in stacks], axis=0)

        def b_rows(b):
            return jnp.transpose(b, (1, 2, 0)).reshape(-1, rank)

        a_own = rows_a((a_q, a_k, a_v))
        w_own = jnp.concatenate([rows_t(w_q), rows_t(w_k), rows_t(w_v)], axis=0)
        b_own = jnp.concatenate([b_rows(b[a]) for a in range(n_ad) for b in (b_q, b_k, b_v)], axis=0)
        o_own = w_o.reshape(qw, D)
        l_own = jnp.concatenate([a_o.reshape(n_ad * qw, rank), b_o.reshape(n_ad * rank, qw), b_down.reshape(n_ad * rank, qw)], axis=0)
        u_own = rows_a((a_gate, a_up))
        owned = (a_own, w_own, b_own, o_own, l_own, u_own)
        mlp_own = (w_gate, w_up, w_down, b_gate, b_up, a_down)
        mlp_other = tuple(swapped(w) for w in mlp_own)

        inv_freq = ROPE_BASE ** (-2.0 * jnp.arange(half, dtype=F32) / hd)
        ang = jnp.arange(S, dtype=F32)[:, None] * inv_freq[None, :]
        cos, sin = jnp.cos(ang), jnp.sin(ang)
        cos_t, sin_t = cos.T, sin.T

        x4 = x_in.reshape(chips, per, S, D)
        M = chips * S
        Fc = CORES * w_gate.shape[1]
        dma = pltpu.SemaphoreType.DMA
        dw = qw + 2 * hd
        attn_all, _, _, _, g_wo, g_b, g_gu = pl.pallas_call(
            functools.partial(attn_body, (n_dev, seqs, S, hd, nq, rank, D, chips)),
            in_specs=[pl.BlockSpec(memory_space=pltpu.SMEM), ANY] + [pl.BlockSpec(memory_space=pltpu.VMEM)] * 3 + [ANY] * len(owned),
            out_specs=[ANY] * (1 + len(owned)),
            scratch_shapes=[
                pltpu.VMEM((steps, D, M), BF16), pltpu.VMEM((steps, 3 * rank, M), BF16), pltpu.VMEM((steps, M, n_dev * qw), BF16),
                pltpu.VMEM((chips, CORES * dw, D), BF16), pltpu.VMEM((chips, n_ad, CORES * dw, rank), BF16),
                pltpu.VMEM((2, CORES * qw, M), BF16), pltpu.VMEM((2, CORES, M, hd), BF16), pltpu.VMEM((2, CORES * hd, M), BF16),
                dma((n_dev, 3 * n_ad)), dma((chips, CORES, 1 + n_ad)), dma((2, chips)), dma((steps,)), dma((len(owned), 8)), dma((len(owned), 8))],
            out_shape=[jax.ShapeDtypeStruct((steps, M, n_dev * qw), BF16)] + [
                jax.ShapeDtypeStruct((n_dev,) + v.shape, BF16) for v in owned],
            compiler_params=pltpu.CompilerParams(vmem_limit_bytes=VMEM_LIMIT, collective_id=1, has_side_effects=True),
            name="attn_ring",
            cost_estimate=pl.CostEstimate(flops=3 * steps * M * D * (n_dev * qw + 2 * n_dev * hd + 3 * rank),
                                          bytes_accessed=6 * steps * M * D + 33 * 2**20, transcendentals=0),
        )(adapter_ids, x4, gain_attn.reshape(1, D), cos_t, sin_t, *owned)
        me = lax.axis_index('tensor')
        g_wo, g_b, g_gu = [lax.dynamic_update_slice(g, own[None], (me, 0, 0))
                           for g, own in zip((g_wo, g_b, g_gu), owned[3:])]
        core = me % CORES
        meta = jnp.concatenate([adapter_ids.astype(jnp.int32), core.reshape(1).astype(jnp.int32)])
        x1_all = pl.pallas_call(
            functools.partial(oproj_body, (n_dev, seqs, S, qw, rank, D, chips)),
            grid_spec=pltpu.PrefetchScalarGridSpec(
                num_scalar_prefetch=1, grid=(steps,),
                in_specs=[pl.BlockSpec((1, M, n_dev * qw), lambda i, m: (i, 0, 0)),
                          pl.BlockSpec((chips, 1, S, D), lambda i, m: (0, m[seqs] * steps + i, 0, 0)), ANY, ANY],
                out_specs=pl.BlockSpec((chips, 1, S, D), lambda i, m: (0, i, 0, 0)),
                scratch_shapes=[pltpu.VMEM((n_dev * qw, D), BF16), pltpu.VMEM((n_ad, n_dev * qw, rank), BF16),
                                pltpu.VMEM((n_ad, rank, D), BF16), pltpu.VMEM((M, rank), BF16), dma((1,))]),
            out_shape=jax.ShapeDtypeStruct((chips, steps, S, D), BF16),
            compiler_params=pltpu.CompilerParams(vmem_limit_bytes=VMEM_LIMIT, dimension_semantics=("arbitrary",)), name="oproj",
            cost_estimate=pl.CostEstimate(flops=2 * steps * M * D * (D + 2 * rank),
                                          bytes_accessed=6 * steps * M * D + 12 * 2**20, transcendentals=0),
        )(meta, attn_all, x4, g_wo.reshape(n_dev * qw, D), g_b)
        pairs = [w for own, other in zip(mlp_own, mlp_other) for w in (own, other)]
        y = pl.pallas_call(
            functools.partial(mlp_body, (seqs, S, rank, D, chips)),
            in_specs=[pl.BlockSpec(memory_space=pltpu.SMEM), ANY, pl.BlockSpec(memory_space=pltpu.VMEM)] + [ANY] * 14,
            out_specs=ANY,
            scratch_shapes=[
                pltpu.VMEM((D, Fc), BF16), pltpu.VMEM((D, Fc), BF16), pltpu.VMEM((Fc, D), BF16),
                pltpu.VMEM((n_ad, rank, Fc), BF16), pltpu.VMEM((n_ad, rank, Fc), BF16),
                pltpu.VMEM((n_ad, 2 * rank, D), BF16), pltpu.VMEM((n_ad, Fc, rank), BF16), pltpu.VMEM((n_ad, rank, D), BF16),
                pltpu.VMEM((2, chips, S, D), BF16), pltpu.VMEM((M, D), BF16), pltpu.VMEM((M, 2 * rank), BF16), pltpu.VMEM((M, Fc), BF16),
                pltpu.VMEM((3, chips, S, D + rank), BF16), pltpu.VMEM((2, 4, S // 2, D + rank), BF16),
                pltpu.VMEM((2, 3, S, D + rank), BF16), pltpu.VMEM((2, S, D), BF16), pltpu.VMEM((2, S, D), BF16),
                dma((12 + n_dev * n_ad * 3,)), dma((4,)), dma((2,)), dma((2, steps)), dma((2, steps)), dma((2, steps)), dma((2, steps)),
                dma((2, steps)), dma((2, steps)), dma((2, steps)), dma((2, steps)), dma((4, steps)), dma((4, steps))],
            out_shape=jax.ShapeDtypeStruct((n_dev, steps, S, D), BF16),
            compiler_params=pltpu.CompilerParams(vmem_limit_bytes=VMEM_LIMIT, collective_id=0, has_side_effects=True),
            name="mlp_ring",
            cost_estimate=pl.CostEstimate(flops=2 * steps * M * D * (3 * Fc + 4 * rank),
                                          bytes_accessed=8 * steps * M * D + 34 * 2**20, transcendentals=steps * M * Fc),
        )(adapter_ids, x1_all, gain_mlp.reshape(1, D), g_gu, *pairs, g_b)
        return y.reshape(seqs, S, D)

    return jax.shard_map(local_layer, mesh=mesh, in_specs=in_specs, out_specs=P('data', None, None), check_vma=False)
```
